32 devices in a mesh: seq: 8 (over y, x, core), dp: 4 (over z).
Axes of the slice: x: 2, y: 2, z: 4, core: 2. Of those that a mesh axis runs over, the one named last changes fastest.
Arguments:
- queries: bfloat16 [4, 3072, 2048], P('dp', 'seq'), may hold values from -40 to 40
- keys: bfloat16 [4, 3072, 2048], P('dp', 'seq'), may hold values from -40 to 40
- values: bfloat16 [4, 3072, 2048], P('dp', 'seq'), may hold values from -6 to 6
- out_grad: bfloat16 [4, 3072, 2048], P('dp', 'seq'), may hold values from -6 to 6
- proj_weight: bfloat16 [2048, 2048], P('dp'), may hold values from -0.125 to 0.125
- lengths: int32 [4], P('dp'), may hold values from 768 to 3072
Outputs:
- query_grad: bfloat16 [4, 3072, 2048], P('dp', 'seq')
- key_grad: bfloat16 [4, 3072, 2048], P('dp', 'seq')
- value_grad: bfloat16 [4, 3072, 2048], P('dp', 'seq')
- weight_grad: float32 [2048, 2048], P('dp', 'seq')
The draws below stay inside these ranges and needn't reach their ends.
All inputs are finite; a program needn't handle non-finite values.
Results may differ from the reference program's by a relative error of at most 0.019.
Values may be sent and summed in bfloat16 or wider, within the bound.
A program may use at most 192 MiB of HBM per device.

```python
import jax
import jax.numpy as jnp
from jax import lax

HEADS = 16
HEAD_DIM = 128
DW = 2048
CYCLE = 2
TOK_DEV = 384
FEAT = 2048
TOKENS = 3072
SEQS = 4
N_SEQ = 8


def paired_rows(key):
    base = jax.random.fold_in(key, 7)
    query_draw = jax.random.normal(jax.random.fold_in(base, 1), (SEQS, TOKENS, FEAT), jnp.float32)
    key_draw = jax.random.normal(jax.random.fold_in(base, 2), (SEQS, TOKENS, FEAT), jnp.float32)
    query_draw = jnp.clip(query_draw, -40.0, 40.0)
    key_draw = jnp.clip(key_draw, -40.0, 40.0)
    return (query_draw, key_draw)


def draw_queries(key, part):
    return paired_rows(key)[0].astype(jnp.bfloat16)


def draw_keys(key, part):
    return paired_rows(key)[1].astype(jnp.bfloat16)


def with_ends(values, stream_key, smallest, largest):
    index_at = [jax.random.randint(jax.random.fold_in(stream_key, axis), (), 0, length) for axis, length in enumerate(values.shape)]
    longest = values.shape.index(max(values.shape))
    next_to = index_at[:longest] + [(index_at[longest] + 1) % values.shape[longest]] + index_at[longest + 1:]
    return values.at[tuple(index_at)].set(smallest).at[tuple(next_to)].set(largest)


def strengthened(values, own_key, source, target, shards_of, factor):
    owner, partner = [(jnp.arange(values.shape[dim]) // (values.shape[dim] // shards_of)).reshape([-1 if axis == dim else 1 for axis in range(values.ndim)]) for dim in (source, target)]
    chosen = jax.random.permutation(own_key, shards_of)[partner]
    strong = (owner == chosen) | (owner == (partner + shards_of // 2) % shards_of)
    return jnp.where(strong, factor * values, values)


def level_of(key, extent, pieces, smallest, high):
    gain = 1.0
    for dim, blocks in pieces:
        draws = jax.random.uniform(jax.random.fold_in(jax.random.fold_in(key, 6), dim), (blocks,), jnp.float32, smallest / len(pieces), high / len(pieces))
        gain = gain * jnp.repeat(jnp.exp(draws), extent[dim] // blocks).reshape((-1,) + (1,) * (len(extent) - 1 - dim))
    return gain


def bell_draw(stream_key, dims, spread, most, cuts=(), held_as=jnp.bfloat16):
    drawn = spread * jax.random.normal(stream_key, dims, jnp.float32)
    if cuts:
        drawn = drawn * level_of(stream_key, dims, cuts, -0.22, 0.18)
    return jnp.clip(drawn, -most, most).astype(held_as)


def heavy_noise(rng, shape, deviation, bound, shards, heavy, held_as=jnp.bfloat16):
    drawn = deviation * jax.random.normal(rng, shape, jnp.float32)
    if shards:
        drawn = drawn * level_of(rng, shape, shards, -0.22, 0.18)
    return jnp.clip(strengthened(drawn, jax.random.fold_in(rng, 3), *heavy), -bound, bound).astype(held_as)


def setup_inputs(seed: int = 0) -> dict:
    arg_keys = jax.random.split(jax.random.key(seed), 7)
    return {
        "queries": draw_queries(jax.random.fold_in(arg_keys[6], 71), 0),
        "keys": draw_keys(jax.random.fold_in(arg_keys[6], 71), 0),
        "values": bell_draw(arg_keys[2], (SEQS, TOKENS, FEAT), 1.0, 6.0, ((0, 4), (1, 8))),
        "out_grad": heavy_noise(arg_keys[3], (SEQS, TOKENS, DW), 1.0, 6.0, ((0, 4), (1, 8)), (1, 2, 8, 2.0)),
        "proj_weight": bell_draw(arg_keys[4], (FEAT, DW), FEAT ** -0.5, 0.125, ((0, 4),)),
        "lengths": with_ends(jax.random.randint(arg_keys[5], (SEQS,), TOKENS // 4, TOKENS + 1), jax.random.fold_in(arg_keys[5], 1), TOKENS // 4, TOKENS).astype(jnp.int32),
    }


def reference(queries, keys, values, out_grad, proj_weight, lengths):
    scale = HEAD_DIM ** -0.5
    window = (CYCLE + 1) * TOK_DEV
    leading = CYCLE * TOK_DEV
    weight_total = jnp.zeros((FEAT, DW), jnp.float32)
    query_list = []
    key_list = []
    value_list = []
    for batch in range(SEQS):
        query_seq = queries[batch]
        grad_seq = out_grad[batch]
        front = jnp.zeros((leading, FEAT), jnp.bfloat16)
        key_padded = jnp.concatenate([front, keys[batch]], 0)
        value_padded = jnp.concatenate([front, values[batch]], 0)
        limit = lengths[batch]

        def block_step(carry, index):
            key_accum, value_accum, weight_accum = carry
            first = (index * TOK_DEV).astype(jnp.int32)
            query_block = lax.dynamic_slice_in_dim(query_seq, first, TOK_DEV, 0)
            grad_block = lax.dynamic_slice_in_dim(grad_seq, first, TOK_DEV, 0)
            key_window = lax.dynamic_slice_in_dim(key_padded, first, window, 0)
            value_window = lax.dynamic_slice_in_dim(value_padded, first, window, 0)
            query_pos = first + jnp.arange(TOK_DEV, dtype=jnp.int32)
            key_pos = first - leading + jnp.arange(window, dtype=jnp.int32)
            allowed = (key_pos[None, :] >= 0) & (key_pos[None, :] <= query_pos[:, None])
            query_heads = query_block.reshape(TOK_DEV, HEADS, HEAD_DIM).astype(jnp.float32)
            key_heads = key_window.reshape(window, HEADS, HEAD_DIM).astype(jnp.float32)
            value_heads = value_window.reshape(window, HEADS, HEAD_DIM).astype(jnp.float32)
            scores = jnp.einsum("thd,shd->hts", query_heads, key_heads) * scale
            scores = jnp.where(allowed[None], scores, -1e30)
            maximum = jnp.max(scores, axis=2, keepdims=True)
            lse = maximum + jnp.log(jnp.sum(jnp.exp(scores - maximum), axis=2, keepdims=True))
            probs = jnp.exp(scores - lse)
            probs_b = probs.astype(jnp.bfloat16)
            attn_out = jnp.einsum("hts,shd->thd", probs_b.astype(jnp.float32), value_heads).astype(jnp.bfloat16)
            live = (query_pos < limit).astype(jnp.bfloat16)
            grad_masked = grad_block * live[:, None]
            out_bwd = jnp.dot(grad_masked, proj_weight.T, preferred_element_type=jnp.float32).astype(jnp.bfloat16)
            attn_flat = attn_out.reshape(TOK_DEV, FEAT)
            weight_accum = weight_accum + lax.dot_general(attn_flat, grad_masked, (((0,), (0,)), ((), ())), preferred_element_type=jnp.float32)
            out_heads = out_bwd.reshape(TOK_DEV, HEADS, HEAD_DIM).astype(jnp.float32)
            delta = jnp.sum(out_heads * attn_out.astype(jnp.float32), axis=2)
            prob_grad = jnp.einsum("thd,shd->hts", out_heads, value_heads)
            score_grad = (probs * (prob_grad - delta.T[:, :, None]) * scale).astype(jnp.bfloat16)
            score_f = score_grad.astype(jnp.float32)
            query_grad = jnp.einsum("hts,shd->thd", score_f, key_heads).astype(jnp.bfloat16)
            key_term = jnp.einsum("hts,thd->shd", score_f, query_heads).astype(jnp.bfloat16)
            value_term = jnp.einsum("hts,thd->shd", probs_b.astype(jnp.float32), out_heads).astype(jnp.bfloat16)
            key_old = lax.dynamic_slice_in_dim(key_accum, first, window, 0)
            value_old = lax.dynamic_slice_in_dim(value_accum, first, window, 0)
            key_accum = lax.dynamic_update_slice_in_dim(key_accum, key_old + key_term.reshape(window, FEAT).astype(jnp.float32), first, 0)
            value_accum = lax.dynamic_update_slice_in_dim(value_accum, value_old + value_term.reshape(window, FEAT).astype(jnp.float32), first, 0)
            return (key_accum, value_accum, weight_accum), query_grad.reshape(TOK_DEV, FEAT)

        start_carry = (jnp.zeros((TOKENS + leading, FEAT), jnp.float32), jnp.zeros((TOKENS + leading, FEAT), jnp.float32), weight_total)
        final_carry, query_blocks = lax.scan(block_step, start_carry, jnp.arange(N_SEQ, dtype=jnp.int32))
        key_accum, value_accum, weight_total = final_carry
        query_list.append(query_blocks.reshape(TOKENS, FEAT))
        key_list.append(key_accum[leading:].astype(jnp.bfloat16))
        value_list.append(value_accum[leading:].astype(jnp.bfloat16))
    return (jnp.stack(query_list), jnp.stack(key_list), jnp.stack(value_list), weight_total)
```

```python
import functools

import jax
import jax.numpy as jnp
from jax import lax
from jax.experimental import pallas as pl
from jax.experimental.pallas import tpu as pltpu
from jax.sharding import PartitionSpec as P

HEAD_DIM = 128
PAIR = 2 * HEAD_DIM
LOG2E = 1.4426950408889634
NEG = -1e30
MESH = pl.DeviceIdType.MESH

NT = (((1,), (1,)), ((), ()))
NN = (((1,), (0,)), ((), ()))
TN = (((0,), (0,)), ((), ()))


def dot(a, b, dims):
    return lax.dot_general(a, b, dims, preferred_element_type=jnp.float32)


def flip(i, bit):
    return i + bit - 2 * bit * lax.rem(i // bit, 2)


def shard_order(count):
    return [sorted(range(count), key=lambda d: (abs(d - z), d < z)) for z in range(count)]


def pick(table, z, s):
    found = jnp.int32(0)
    for zz, row in enumerate(table):
        for ss, value in enumerate(row):
            found = found + jnp.where(z == zz, jnp.where(s == ss, value, 0), 0)
    return found


def every(count, body):
    def step(index, carry):
        body(index)
        return carry

    lax.fori_loop(0, count, step, 0)


def kernel(n, nd, len_ref, q_hbm, k_hbm, v_hbm, g_hbm, w_hbm, dq_hbm, dk_hbm, dv_hbm, wg_hbm, *scratch):
    (
        q_buf, kv, far, near, t0, t1in, behind, relay, do_buf, dq_buf, o_buf, o_in,
        g_buf, g_mine, g_send, g_in, w_buf, y_send, y_in, z_buf, z_in, kept, acc, x_send, x_in, out_buf,
        q_l, kv_l, g_l, w_l, dq_s, out_s,
        far_s, far_r, near_s, near_r, t1_s, t1_r, ret_s, ret_r, rel_s, rel_r,
        o_s, o_r, g_s, g_r, wu_s, wd_s, w_r, wp_s, wp_r, y_s, y_r, z_s, z_r, x_s, x_r,
    ) = scratch
    f32, bf16 = jnp.float32, jnp.bfloat16
    i, z = lax.axis_index("seq"), lax.axis_index("dp")
    steps, _, _, tokens, _ = kv.shape
    per = steps // nd
    chips = n // 2
    chip = i // 2
    par = lax.rem(i, 2)
    mate = flip(i, 1)
    ahead, back = lax.rem(i + 2, n), lax.rem(i + n - 2, n)
    across = flip(i, n // 2)
    beside = flip(i, 2)
    relayed = n == 8
    width = w_hbm.shape[1]
    half = width // 2
    own = width // n
    span = half // 2
    table = shard_order(nd)

    def pair_at(it):
        return pick(table, z, it // per) * per + lax.rem(it, per)

    def rdma(src, dst, send, recv, **where):
        return pltpu.make_async_remote_copy(
            src_ref=src, dst_ref=dst, send_sem=send, recv_sem=recv, device_id=where, device_id_type=MESH
        )

    def columns(start, size):
        return pl.ds(pl.multiple_of(start, 128), size)

    def load_kv(it):
        at = pair_at(it) * PAIR
        for a in range(2):
            for b, ref in enumerate((k_hbm, v_hbm)):
                src = ref.at[:, columns(at + a * HEAD_DIM, HEAD_DIM)]
                pltpu.make_async_copy(src, kv.at[it, a, b], kv_l.at[it]).start()

    def load_q(it):
        at = pair_at(it) * PAIR
        for a in range(2):
            src = q_hbm.at[:, columns(at + a * HEAD_DIM, HEAD_DIM)]
            pltpu.make_async_copy(src, q_buf.at[it, a], q_l.at[it]).start()

    every(steps, load_kv)
    load_g = pltpu.make_async_copy(g_hbm, g_buf, g_l.at[0])
    load_g.start()
    own_w = []
    for k in range(per):
        for h in range(2):
            src = w_hbm.at[pl.ds(k * PAIR, PAIR), pl.ds(h * half, half)]
            own_w.append(pltpu.make_async_copy(src, w_buf.at[z * per + k, h], w_l.at[2 * k + h]))
            own_w[-1].start()
    every(steps, load_q)

    bits = []
    bit = n // 2
    while bit > 1:
        bits.append(bit)
        bit //= 2
    greet = [dict(seq=mate), dict(seq=ahead), dict(seq=back)]
    greet += [dict(seq=flip(i, b)) for b in bits]
    greet += [dict(dp=lax.rem(z + s, nd)) for s in range(1, nd)]
    barrier = pltpu.get_barrier_semaphore()
    for who in greet:
        pl.semaphore_signal(barrier, inc=1, device_id=who, device_id_type=MESH)

    @pl.when(chip == 0)
    def _():
        def clear(it):
            far[it] = jnp.zeros_like(far[it])

        every(steps, clear)

    pl.semaphore_wait(barrier, len(greet))

    def far_copy(it, a):
        return rdma(kv.at[it, a], far.at[it, a], far_s.at[2 * it + a], far_r.at[2 * it + a], seq=ahead)

    def far_relay_in(it):
        return rdma(kv.at[it, 1], relay.at[it], far_s.at[2 * it + 1], rel_r.at[it], seq=across)

    def far_relay_out(it):
        return rdma(relay.at[it], far.at[it, 1], rel_s.at[it], far_r.at[2 * it + 1], seq=beside)

    def ret_copy(it, a):
        return rdma(far.at[it, a], behind.at[it, a], ret_s.at[2 * it + a], ret_r.at[2 * it + a], seq=back)

    def ret_relay_in(it):
        return rdma(far.at[it, 1], relay.at[it], ret_s.at[2 * it + 1], rel_r.at[it], seq=across)

    def ret_relay_out(it):
        return rdma(relay.at[it], behind.at[it, 1], rel_s.at[it], ret_r.at[2 * it + 1], seq=beside)

    def near_copy(src, it, a):
        return rdma(src.at[it, a], near.at[it, a], near_s.at[2 * it + a], near_r.at[2 * it + a], seq=mate)

    def t1_copy(it, a):
        return rdma(near.at[it, a], t1in.at[it, a], t1_s.at[2 * it + a], t1_r.at[2 * it + a], seq=mate)

    def o_copy(it):
        return rdma(o_buf.at[it], o_in.at[it], o_s.at[it], o_r.at[it], seq=mate)

    def w_up(piece):
        return rdma(w_buf.at[piece, par], w_buf.at[piece, par], wu_s.at[piece], w_r.at[piece], dp=lax.rem(z + 1, nd))

    def w_down(piece):
        return rdma(w_buf.at[piece, par], w_buf.at[piece, par], wd_s.at[piece], w_r.at[piece], dp=lax.rem(z + nd - 1, nd))

    def w_mate(piece, side):
        return rdma(w_buf.at[piece, side], w_buf.at[piece, side], wp_s.at[piece], wp_r.at[piece], seq=mate)

    def y_copy(it):
        return rdma(y_send.at[it], y_in.at[it], y_s.at[it], y_r.at[it], seq=across)

    def z_copy(it, source, shard):
        k = lax.rem(it, per)
        return rdma(z_buf.at[it], z_in.at[source, k], z_s.at[it], z_r.at[source * per + k], dp=shard)

    def first_sends(it):
        pltpu.make_async_copy(kv.at[it], kv.at[it], kv_l.at[it]).wait()

        @pl.when(chip < chips - 1)
        def _():
            far_copy(it, 0).start()
            if relayed:
                pl.when(chip != 1)(lambda: far_copy(it, 1).start())
                pl.when(chip == 1)(lambda: far_relay_in(it).start())
            else:
                far_copy(it, 1).start()

        @pl.when(par == 0)
        def _():
            for a in range(2):
                near_copy(kv, it, a).start()

    every(steps, first_sends)

    for copy in own_w:
        copy.wait()
    for k in range(per):
        pl.when(z < nd - 1)(lambda: w_up(z * per + k).start())
        pl.when(z > 0)(lambda: w_down(z * per + k).start())

    load_g.wait()
    at_row = i * tokens + lax.broadcasted_iota(jnp.int32, (tokens, 1), 0)
    live = at_row < len_ref[0]
    for c in range(chips):
        first = g_buf[:, 2 * c * own : (2 * c + 1) * own].astype(f32)
        second = g_buf[:, (2 * c + 1) * own : (2 * c + 2) * own].astype(f32)
        first, second = jnp.where(live, first, 0.0), jnp.where(live, second, 0.0)
        g_buf[:, 2 * c * own : (2 * c + 2) * own] = jnp.concatenate([first, second], 1).astype(bf16)
        g_mine[c * own : (c + 1) * own, :] = jnp.where(par == 0, first, second).T.astype(bf16)
        g_send[c * own : (c + 1) * own, :] = jnp.where(par == 0, second, first).T.astype(bf16)
    g_copy = rdma(g_send, g_in, g_s.at[0], g_r.at[0], seq=mate)
    g_copy.start()

    def halo_relay(it):
        far_relay_in(it).wait_recv()
        far_relay_out(it).start()

    if relayed:
        pl.when(chip == chips - 1)(lambda: halo_relay(0))

    g_copy.wait_recv()
    scale = HEAD_DIM ** (-0.5)
    c_exp = scale * LOG2E

    def begin(it):
        @pl.when(chip > 0)
        def _():
            for a in range(2):
                far_copy(it, a).wait_recv()

        @pl.when(par == 1)
        def _():
            for a in range(2):
                near_copy(far, it, a).start()

        if relayed:
            for extra in (1, 2):

                @pl.when(jnp.logical_and(chip == chips - 1, 2 * it + extra < steps))
                def _():
                    halo_relay(2 * it + extra)

        piece = pair_at(it)

        @pl.when(it >= per)
        def _():
            w_mate(piece, 1 - par).wait_recv()

        do = dot(g_buf[:, :half], w_buf[piece, 0], NT) + dot(g_buf[:, half:], w_buf[piece, 1], NT)
        do_buf[...] = do.astype(bf16)

    def attend(it):
        causal_keys = lax.broadcasted_iota(jnp.int32, (tokens, tokens), 0)
        causal_queries = lax.broadcasted_iota(jnp.int32, (tokens, tokens), 1)
        for a in range(2):
            near_copy(kv, it, a).wait_recv()
            q = q_buf[it, a]
            sources = (kv, near, far)
            parts, tops = [], []
            for offset, source in enumerate(sources):
                s = dot(source[it, a, 0], q, NT)
                if offset == 0:
                    s = jnp.where(causal_keys <= causal_queries, s, NEG)
                parts.append(s)
                top = jnp.max(s, axis=0, keepdims=True)
                if offset:
                    top = top + jnp.where(i >= offset, 0.0, NEG)
                tops.append(top)
            top = functools.reduce(jnp.maximum, tops) * c_exp
            total = None
            for offset in range(3):
                shift = top if offset == 0 else top + jnp.where(i >= offset, 0.0, -NEG)
                parts[offset] = jnp.exp2(parts[offset] * c_exp - shift)
                t = jnp.sum(parts[offset], axis=0, keepdims=True)
                total = t if total is None else total + t
            inverse = 1.0 / total
            out = None
            for offset, source in enumerate(sources):
                parts[offset] = parts[offset] * inverse
                o = dot(source[it, a, 1], parts[offset].astype(bf16), TN)
                out = o if out is None else out + o
            o = out.T.astype(bf16)
            o_buf[it, :, a * HEAD_DIM : (a + 1) * HEAD_DIM] = o
            do = do_buf[:, a * HEAD_DIM : (a + 1) * HEAD_DIM]
            delta = jnp.sum((do.astype(f32) * o.astype(f32)).T, axis=0, keepdims=True)
            near_copy(kv, it, a).wait_send()
            dq = None
            for offset, (source, term) in enumerate(zip(sources, (t0, near, far))):
                k, v = source[it, a, 0], source[it, a, 1]
                p = parts[offset]
                dv = dot(p.astype(bf16), do, NN)
                ds = (p * (dot(v, do, NT) - delta)).astype(bf16)
                dk = dot(ds, q, NN) * scale
                part = dot(k, ds, TN)
                dq = part if dq is None else dq + part
                term[it, a, 0] = dk.astype(bf16)
                term[it, a, 1] = dv.astype(bf16)
                if offset == 1:
                    t1_copy(it, a).start()
            dq_buf[it, :, a * HEAD_DIM : (a + 1) * HEAD_DIM] = (dq * scale).T.astype(bf16)
        o_copy(it).start()
        pltpu.make_async_copy(dq_buf.at[it], dq_hbm.at[:, columns(pair_at(it) * PAIR, PAIR)], dq_s.at[it]).start()

    def move_weights(it):
        j = it - 1
        below, above = z - 1 - j // per, z + 1 + j // per

        @pl.when(jnp.logical_and(it >= 1, below >= 0))
        def _():
            piece = below * per + lax.rem(j, per)
            w_up(piece).wait_recv()
            pl.when(z < nd - 1)(lambda: w_up(piece).start())
            w_mate(piece, par).start()

        @pl.when(jnp.logical_and(it >= 1, above <= nd - 1))
        def _():
            piece = above * per + lax.rem(j, per)
            w_down(piece).wait_recv()
            pl.when(z > 0)(lambda: w_down(piece).start())
            w_mate(piece, par).start()

    high = lax.rem(i // bits[0], 2)

    def stage_a(m):
        for a in range(2):
            t1_copy(m, a).wait_recv()

            @pl.when(par == 1)
            def _():
                far[m, a] = (far[m, a].astype(f32) + t1in[m, a].astype(f32)).astype(bf16)

        @pl.when(chip > 0)
        def _():
            ret_copy(m, 0).start()
            if relayed:
                pl.when(chip != 2)(lambda: ret_copy(m, 1).start())
                pl.when(chip == 2)(lambda: ret_relay_in(m).start())
            else:
                ret_copy(m, 1).start()

        o_copy(m).wait_recv()

        def product(side):
            rows = pl.ds(pl.multiple_of(side * span, span), span)
            return dot(g_mine[rows, :], o_buf[m], NN) + dot(g_in[rows, :], o_in[m], NN)

        y_send[m] = product(1 - high).astype(bf16)
        y_copy(m).start()
        kept[lax.rem(m, 2)] = product(high)

    def stage_b(m):
        y_copy(m).wait_recv()
        total = kept[lax.rem(m, 2)] + y_in[m].astype(f32)

        @pl.when(m < per)
        def _():
            acc[lax.rem(m, per)] = total

        @pl.when(m >= per)
        def _():
            z_buf[m] = total.astype(bf16)
            z_copy(m, z, pick(table, z, m // per)).start()

        if relayed:

            @pl.when(chip == 0)
            def _():
                ret_relay_in(m).wait_recv()
                ret_relay_out(m).start()

    def step(it):
        pl.when(it < steps)(lambda: begin(it))
        pl.when(jnp.logical_and(it >= 1, it <= steps))(lambda: stage_a(it - 1))
        pl.when(it >= 2)(lambda: stage_b(it - 2))

        @pl.when(it < steps)
        def _():
            pltpu.make_async_copy(q_buf.at[it], q_buf.at[it], q_l.at[it]).wait()
            attend(it)
            pl.when(it < steps - 1)(lambda: move_weights(it))

    every(steps + 2, step)

    def finish(m):
        @pl.when(chip < chips - 1)
        def _():
            for a in range(2):
                ret_copy(m, a).wait_recv()

        for a in range(2):
            for b, out in enumerate((dk_hbm, dv_hbm)):
                total = t0[m, a, b].astype(f32)
                total = total + jnp.where(par == 0, t1in[m, a, b].astype(f32), 0.0)
                total = total + jnp.where(chip < chips - 1, behind[m, a, b].astype(f32), 0.0)
                t0[m, a, b] = total.astype(bf16)
                dst = out.at[:, columns(pair_at(m) * PAIR + a * HEAD_DIM, HEAD_DIM)]
                pltpu.make_async_copy(t0.at[m, a, b], dst, out_s.at[m]).start()

    every(steps - 1, finish)

    for s in range(1, nd):
        source = lax.rem(z + s, nd)
        for k in range(per):
            z_copy(per + k, source, z).wait_recv()
            acc[k] = acc[k] + z_in[source, k].astype(f32)
    base = jnp.int32(0)
    rows = span
    sent = []
    for level, b in enumerate(bits[1:]):
        rows //= 2
        up = lax.rem(i // b, 2)
        away = pl.ds(pl.multiple_of(base + (1 - up) * rows, rows), rows)
        base = base + up * rows
        stay = pl.ds(pl.multiple_of(base, rows), rows)
        at = pl.ds(span - 2 * rows, rows)
        for k in range(per):
            x_send[k, at, :] = acc[k, away, :].astype(bf16)
            sent.append(
                rdma(
                    x_send.at[k, at, :], x_in.at[k, at, :],
                    x_s.at[level * per + k], x_r.at[level * per + k], seq=flip(i, b),
                )
            )
            sent[-1].start()
        if level == 0:
            finish(steps - 1)
        for k in range(per):
            sent[-per + k].wait_recv()
            acc[k, stay, :] = acc[k, stay, :] + x_in[k, at, :].astype(f32)
    mine = pl.ds(pl.multiple_of(base, own), own)
    for k in range(per):
        out_buf[k * PAIR : (k + 1) * PAIR, :] = acc[k, mine, :].T
    put = pltpu.make_async_copy(out_buf, wg_hbm, g_l.at[0])
    put.start()

    def settle(m):
        for a in range(2):
            pl.when(chip < chips - 1)(lambda: far_copy(m, a).wait_send())
            pl.when(chip > 0)(lambda: ret_copy(m, a).wait_send())
            t1_copy(m, a).wait_send()
        if relayed:
            pl.when(chip == 0)(lambda: ret_relay_out(m).wait_send())
            pl.when(chip == chips - 1)(lambda: far_relay_out(m).wait_send())
        o_copy(m).wait_send()
        y_copy(m).wait_send()

        @pl.when(m >= per)
        def _():
            z_copy(m, z, pick(table, z, m // per)).wait_send()
            w_mate(pair_at(m), par).wait_send()

        pl.when(jnp.logical_and(z < nd - 1, m < (z + 1) * per))(lambda: w_up(m).wait_send())
        pl.when(jnp.logical_and(z > 0, m >= z * per))(lambda: w_down(m).wait_send())
        pltpu.make_async_copy(dq_buf.at[m], dq_hbm.at[:, columns(pair_at(m) * PAIR, PAIR)], dq_s.at[m]).wait()
        pltpu.make_async_copy(t0.at[m], t0.at[m], out_s.at[m]).wait()

    every(steps, settle)
    g_copy.wait_send()
    for copy in sent:
        copy.wait_send()
    put.wait()


def layer(n, nd, queries, keys, values, out_grad, proj_weight, lengths):
    f32, bf16 = jnp.float32, jnp.bfloat16
    tokens, feat = queries.shape[1:]
    rows, width = proj_weight.shape
    steps = feat // PAIR
    per = rows // PAIR
    half = width // 2
    span = half // 2
    own = width // n
    head = (steps, 2, tokens, HEAD_DIM)
    both = (steps, 2, 2, tokens, HEAD_DIM)
    pair = (steps, tokens, PAIR)
    levels = max(1, n.bit_length() - 3)
    vmem = [
        (head, bf16),
        *[(both, bf16)] * 6,
        ((steps, 2, tokens, HEAD_DIM), bf16),
        ((tokens, PAIR), bf16),
        *[(pair, bf16)] * 3,
        ((tokens, width), bf16),
        *[((half, tokens), bf16)] * 3,
        ((steps, 2, PAIR, half), bf16),
        *[((steps, span, PAIR), bf16)] * 3,
        ((nd, per, span, PAIR), bf16),
        ((2, span, PAIR), f32),
        ((per, span, PAIR), f32),
        *[((per, span, PAIR), bf16)] * 2,
        ((rows, own), f32),
    ]
    sems = [steps, steps, 1, 2 * per, steps, steps]
    sems += [2 * steps] * 8 + [steps] * 2
    sems += [steps, steps, 1, 1] + [steps] * 5 + [steps] * 3 + [nd * per] + [levels * per] * 2
    anywhere = pl.BlockSpec(memory_space=pl.ANY)
    grad = jax.ShapeDtypeStruct((tokens, feat), bf16)
    dq, dk, dv, wg = pl.pallas_call(
        functools.partial(kernel, n, nd),
        in_specs=[pl.BlockSpec(memory_space=pltpu.SMEM)] + [anywhere] * 5,
        out_specs=[anywhere] * 4,
        out_shape=[grad, grad, grad, jax.ShapeDtypeStruct((rows, own), f32)],
        scratch_shapes=[pltpu.VMEM(*spec) for spec in vmem] + [pltpu.SemaphoreType.DMA((s,)) for s in sems],
        compiler_params=pltpu.CompilerParams(
            collective_id=0, has_side_effects=True, vmem_limit_bytes=67043328
        ),
        name="banded_backward",
    )(lengths, queries[0], keys[0], values[0], out_grad[0], proj_weight)
    return dq[None], dk[None], dv[None], wg


def solution(mesh):
    rows = P("dp", "seq", None)
    return jax.shard_map(
        functools.partial(layer, mesh.shape["seq"], mesh.shape["dp"]),
        mesh=mesh,
        in_specs=(rows, rows, rows, rows, P("dp", None), P("dp")),
        out_specs=(rows, rows, rows, P("dp", "seq")),
        check_vma=False,
    )
```

```python
import functools

import jax
import jax.numpy as jnp
from jax import lax
from jax.experimental import pallas as pl
from jax.experimental.pallas import tpu as pltpu
from jax.sharding import PartitionSpec as P

HEAD_DIM = 128
PAIR = 2 * HEAD_DIM
LOG2E = 1.4426950408889634
NEG = -1e30
LAG = 5
MESH = pl.DeviceIdType.MESH

NT = (((1,), (1,)), ((), ()))
NN = (((1,), (0,)), ((), ()))
TN = (((0,), (0,)), ((), ()))


def dot(a, b, dims):
    return lax.dot_general(a, b, dims, preferred_element_type=jnp.float32)


def flip(i, bit):
    return i + bit - 2 * bit * lax.rem(i // bit, 2)


def pair_order(count, per):
    orders = []
    for z in range(count):
        shards = sorted(range(count), key=lambda d: (abs(d - z), d < z))
        pairs = [d * per + k for d in shards for k in range(per)]
        if 0 < z < count - 1:
            pairs = pairs[:1] + pairs[per:] + pairs[1:per]
        orders.append(pairs)
    return orders


def pick(table, z, s):
    found = jnp.int32(0)
    for zz, row in enumerate(table):
        for ss, value in enumerate(row):
            found = found + jnp.where(z == zz, jnp.where(s == ss, value, 0), 0)
    return found


def every(count, body):
    def step(index, carry):
        body(index)
        return carry

    lax.fori_loop(0, count, step, 0)


def kernel(n, nd, len_ref, q_hbm, k_hbm, v_hbm, g_hbm, w_hbm, dq_hbm, dk_hbm, dv_hbm, wg_hbm, *scratch):
    (
        q_buf, kv, far, near, t0, t1in, behind, relay, relay2, do_buf, dq_buf, o_buf, o_in,
        g_buf, g_mine, g_send, g_in, w_buf, y_send, y_in, z_buf, z_in, kept, acc, x_send, x_in, out_buf,
        q_l, kv_l, g_l, w_l, dq_s, out_s,
        far_s, far_r, near_s, near_r, t1_s, t1_r, ret_s, ret_r, rel_s, rel_r, rel2_s, rel2_r,
        o_s, o_r, g_s, g_r, wu_s, wd_s, w_r, wp_s, wp_r, y_s, y_r, z_s, z_r, x_s, x_r,
    ) = scratch
    f32, bf16 = jnp.float32, jnp.bfloat16
    i, z = lax.axis_index("seq"), lax.axis_index("dp")
    steps, _, _, tokens, _ = kv.shape
    per = steps // nd
    chips = n // 2
    chip = i // 2
    par = lax.rem(i, 2)
    mate = flip(i, 1)
    ahead, back = lax.rem(i + 2, n), lax.rem(i + n - 2, n)
    across = flip(i, n // 2)
    beside = flip(i, 2)
    relayed = n == 8 and steps == 8
    width = w_hbm.shape[1]
    half = width // 2
    own = width // n
    span = half // 2
    table = pair_order(nd, per)

    def pair_at(it):
        return pick(table, z, it)

    def rdma(src, dst, send, recv, **where):
        return pltpu.make_async_remote_copy(
            src_ref=src, dst_ref=dst, send_sem=send, recv_sem=recv, device_id=where, device_id_type=MESH
        )

    def columns(start, size):
        return pl.ds(pl.multiple_of(start, 128), size)

    def load_kv(it):
        at = pair_at(it) * PAIR
        for a in range(2):
            for b, ref in enumerate((k_hbm, v_hbm)):
                src = ref.at[:, columns(at + a * HEAD_DIM, HEAD_DIM)]
                pltpu.make_async_copy(src, kv.at[it, a, b], kv_l.at[it]).start()

    def load_q(it):
        at = pair_at(it) * PAIR
        for a in range(2):
            src = q_hbm.at[:, columns(at + a * HEAD_DIM, HEAD_DIM)]
            pltpu.make_async_copy(src, q_buf.at[it, a], q_l.at[it]).start()

    every(steps, load_kv)
    load_g = pltpu.make_async_copy(g_hbm, g_buf, g_l.at[0])
    load_g.start()
    own_w = []
    for k in range(per):
        for h in range(2):
            src = w_hbm.at[pl.ds(k * PAIR, PAIR), pl.ds(h * half, half)]
            own_w.append(pltpu.make_async_copy(src, w_buf.at[z * per + k, h], w_l.at[2 * k + h]))
            own_w[-1].start()
    every(steps, load_q)

    bits = []
    bit = n // 2
    while bit > 1:
        bits.append(bit)
        bit //= 2
    greet = [dict(seq=mate), dict(seq=ahead), dict(seq=back)]
    greet += [dict(seq=flip(i, b)) for b in bits]
    greet += [dict(dp=lax.rem(z + s, nd)) for s in range(1, nd)]
    barrier = pltpu.get_barrier_semaphore()
    for who in greet:
        pl.semaphore_signal(barrier, inc=1, device_id=who, device_id_type=MESH)

    @pl.when(chip == 0)
    def _():
        def clear(it):
            far[it] = jnp.zeros_like(far[it])

        every(steps, clear)

    with jax.named_scope("greet"):
        pl.semaphore_wait(barrier, len(greet))

    def far_copy(it, a):
        return rdma(kv.at[it, a], far.at[it, a], far_s.at[2 * it + a], far_r.at[2 * it + a], seq=ahead)

    def far_relay_in(it):
        return rdma(kv.at[it, 1], relay.at[it], far_s.at[2 * it + 1], rel_r.at[it], seq=across)

    def far_relay_out(it):
        return rdma(relay.at[it], far.at[it, 1], rel_s.at[it], far_r.at[2 * it + 1], seq=beside)

    def ret_copy(it, a):
        return rdma(far.at[it, a], behind.at[it, a], ret_s.at[2 * it + a], ret_r.at[2 * it + a], seq=back)

    def ret_relay_in(it):
        return rdma(far.at[it, 1], relay.at[it], ret_s.at[2 * it + 1], rel_r.at[it], seq=across)

    def ret_relay_out(it):
        return rdma(relay.at[it], behind.at[it, 1], rel_s.at[it], ret_r.at[2 * it + 1], seq=beside)

    def ret_relay2_in(it):
        return rdma(far.at[it, 0], relay2.at[it], ret_s.at[2 * it], rel2_r.at[it], seq=beside)

    def ret_relay2_out(it):
        return rdma(relay2.at[it], behind.at[it, 0], rel2_s.at[it], ret_r.at[2 * it], seq=across)

    def near_copy(src, it, a):
        return rdma(src.at[it, a], near.at[it, a], near_s.at[2 * it + a], near_r.at[2 * it + a], seq=mate)

    def t1_copy(it, a):
        return rdma(near.at[it, a], t1in.at[it, a], t1_s.at[2 * it + a], t1_r.at[2 * it + a], seq=mate)

    def o_copy(it):
        return rdma(o_buf.at[it], o_in.at[it], o_s.at[it], o_r.at[it], seq=mate)

    def w_up(piece):
        return rdma(w_buf.at[piece, par], w_buf.at[piece, par], wu_s.at[piece], w_r.at[piece], dp=lax.rem(z + 1, nd))

    def w_down(piece):
        return rdma(w_buf.at[piece, par], w_buf.at[piece, par], wd_s.at[piece], w_r.at[piece], dp=lax.rem(z + nd - 1, nd))

    def w_mate(piece, side):
        return rdma(w_buf.at[piece, side], w_buf.at[piece, side], wp_s.at[piece], wp_r.at[piece], seq=mate)

    def y_copy(it):
        return rdma(y_send.at[it], y_in.at[it], y_s.at[it], y_r.at[it], seq=across)

    def z_copy(it, source, shard):
        k = lax.rem(pair_at(it), per)
        return rdma(z_buf.at[it], z_in.at[source, k], z_s.at[it], z_r.at[source * per + k], dp=shard)

    def z_arrive(source, k):
        return rdma(z_buf.at[0], z_in.at[source, k], z_s.at[0], z_r.at[source * per + k], dp=source)

    def first_sends(it):
        with jax.named_scope("kv_load"):
            pltpu.make_async_copy(kv.at[it], kv.at[it], kv_l.at[it]).wait()

        @pl.when(chip < chips - 1)
        def _():
            far_copy(it, 0).start()
            if relayed:
                pl.when(chip != 1)(lambda: far_copy(it, 1).start())
                pl.when(chip == 1)(lambda: far_relay_in(it).start())
            else:
                far_copy(it, 1).start()

        @pl.when(par == 0)
        def _():
            for a in range(2):
                near_copy(kv, it, a).start()

    every(steps, first_sends)

    with jax.named_scope("w_load"):
        for copy in own_w:
            copy.wait()
    for k in range(per):
        pl.when(z < nd - 1)(lambda: w_up(z * per + k).start())
        pl.when(z > 0)(lambda: w_down(z * per + k).start())

    with jax.named_scope("g_load"):
        load_g.wait()
    at_row = i * tokens + lax.broadcasted_iota(jnp.int32, (tokens, 1), 0)
    live = at_row < len_ref[0]
    for c in range(chips):
        first = g_buf[:, 2 * c * own : (2 * c + 1) * own].astype(f32)
        second = g_buf[:, (2 * c + 1) * own : (2 * c + 2) * own].astype(f32)
        first, second = jnp.where(live, first, 0.0), jnp.where(live, second, 0.0)
        g_buf[:, 2 * c * own : (2 * c + 2) * own] = jnp.concatenate([first, second], 1).astype(bf16)
        g_mine[c * own : (c + 1) * own, :] = jnp.where(par == 0, first, second).T.astype(bf16)
        g_send[c * own : (c + 1) * own, :] = jnp.where(par == 0, second, first).T.astype(bf16)
    g_copy = rdma(g_send, g_in, g_s.at[0], g_r.at[0], seq=mate)
    g_copy.start()

    def halo_relay(it):
        with jax.named_scope("hrel_wait"):
            far_relay_in(it).wait_recv()
        far_relay_out(it).start()

    if relayed:
        pl.when(chip == chips - 1)(lambda: halo_relay(0))

    with jax.named_scope("g_wait"):
        g_copy.wait_recv()
    scale = HEAD_DIM ** (-0.5)
    c_exp = scale * LOG2E

    def begin(it):
        @pl.when(chip > 0)
        def _():
            with jax.named_scope("far_wait"):
                for a in range(2):
                    far_copy(it, a).wait_recv()

        @pl.when(par == 1)
        def _():
            for a in range(2):
                near_copy(far, it, a).start()

        if relayed:
            for extra in range(2):
                at = 2 * it + extra

                @pl.when(jnp.logical_and(chip == chips - 1, jnp.logical_and(at > 0, at < steps)))
                def _():
                    halo_relay(at)

        piece = pair_at(it)

        @pl.when(piece // per != z)
        def _():
            with jax.named_scope("w_wait"):
                w_mate(piece, 1 - par).wait_recv()

        with jax.named_scope("do"):
            do = dot(g_buf[:, :half], w_buf[piece, 0], NT) + dot(g_buf[:, half:], w_buf[piece, 1], NT)
            do_buf[...] = do.astype(bf16)

    def pass_return(m):
        @pl.when(chip == chips - 1)
        def _():
            with jax.named_scope("rel2_wait"):
                ret_relay2_in(m).wait_recv()
            ret_relay2_out(m).start()

    def attend(it):
        causal_keys = lax.broadcasted_iota(jnp.int32, (tokens, tokens), 0)
        causal_queries = lax.broadcasted_iota(jnp.int32, (tokens, tokens), 1)
        for a in range(2):
            with jax.named_scope("near_wait"):
                near_copy(kv, it, a).wait_recv()
            q = q_buf[it, a]
            sources = (kv, near, far)
            parts, tops = [], []
            for offset, source in enumerate(sources):
                s = dot(source[it, a, 0], q, NT)
                if offset == 0:
                    s = jnp.where(causal_keys <= causal_queries, s, NEG)
                parts.append(s)
                top = jnp.max(s, axis=0, keepdims=True)
                if offset:
                    top = top + jnp.where(i >= offset, 0.0, NEG)
                tops.append(top)
            top = functools.reduce(jnp.maximum, tops) * c_exp
            total = None
            for offset in range(3):
                shift = top if offset == 0 else top + jnp.where(i >= offset, 0.0, -NEG)
                parts[offset] = jnp.exp2(parts[offset] * c_exp - shift)
                t = jnp.sum(parts[offset], axis=0, keepdims=True)
                total = t if total is None else total + t
            inverse = 1.0 / total
            out = None
            for offset, source in enumerate(sources):
                parts[offset] = parts[offset] * inverse
                o = dot(source[it, a, 1], parts[offset].astype(bf16), TN)
                out = o if out is None else out + o
            o = out.T.astype(bf16)
            o_buf[it, :, a * HEAD_DIM : (a + 1) * HEAD_DIM] = o
            do = do_buf[:, a * HEAD_DIM : (a + 1) * HEAD_DIM]
            delta = jnp.sum((do.astype(f32) * o.astype(f32)).T, axis=0, keepdims=True)
            near_copy(kv, it, a).wait_send()
            dq = None
            for offset, (source, term) in enumerate(zip(sources, (t0, near, far))):
                k, v = source[it, a, 0], source[it, a, 1]
                p = parts[offset]
                dv = dot(p.astype(bf16), do, NN)
                ds = (p * (dot(v, do, NT) - delta)).astype(bf16)
                dk = dot(ds, q, NN) * scale
                part = dot(k, ds, TN)
                dq = part if dq is None else dq + part
                term[it, a, 0] = dk.astype(bf16)
                term[it, a, 1] = dv.astype(bf16)
                if offset == 1:
                    t1_copy(it, a).start()
            dq_buf[it, :, a * HEAD_DIM : (a + 1) * HEAD_DIM] = (dq * scale).T.astype(bf16)
            if a == 0:
                pl.when(it < steps - 1)(lambda: move_weights(it))
        o_copy(it).start()
        pltpu.make_async_copy(dq_buf.at[it], dq_hbm.at[:, columns(pair_at(it) * PAIR, PAIR)], dq_s.at[it]).start()

    def move_weights(it):
        ends = jnp.logical_or(z == 0, z == nd - 1)
        j = it - jnp.where(ends, 1, 0)
        below, above = z - 1 - j // per, z + 1 + j // per

        @pl.when(jnp.logical_and(j >= 0, below >= 0))
        def _():
            piece = below * per + lax.rem(j, per)
            with jax.named_scope("up_wait"):
                w_up(piece).wait_recv()
            pl.when(z < nd - 1)(lambda: w_up(piece).start())
            w_mate(piece, par).start()

        @pl.when(jnp.logical_and(j >= 0, above <= nd - 1))
        def _():
            piece = above * per + lax.rem(j, per)
            with jax.named_scope("down_wait"):
                w_down(piece).wait_recv()
            pl.when(z > 0)(lambda: w_down(piece).start())
            w_mate(piece, par).start()

    high = lax.rem(i // bits[0], 2)

    def stage_a(m):
        for a in range(2):
            with jax.named_scope("t1_wait"):
                t1_copy(m, a).wait_recv()

            @pl.when(par == 1)
            def _():
                far[m, a] = (far[m, a].astype(f32) + t1in[m, a].astype(f32)).astype(bf16)

        @pl.when(chip > 0)
        def _():
            if relayed:

                @pl.when(chip != 2)
                def _():
                    ret_copy(m, 0).start()
                    ret_copy(m, 1).start()

            else:
                ret_copy(m, 0).start()
                ret_copy(m, 1).start()

        with jax.named_scope("o_wait"):
            o_copy(m).wait_recv()

        def product(side):
            rows = pl.ds(pl.multiple_of(side * span, span), span)
            return dot(g_mine[rows, :], o_buf[m], NN) + dot(g_in[rows, :], o_in[m], NN)

        with jax.named_scope("wgrad"):
            y_send[m] = product(1 - high).astype(bf16)
            y_copy(m).start()
            kept[lax.rem(m, LAG)] = product(high)

    def send_around(m):
        ret_relay2_in(m).start()
        ret_relay_in(m).start()

    def corner_return(m):
        @pl.when(chip == 0)
        def _():
            with jax.named_scope("rel_wait"):
                ret_relay_in(m).wait_recv()
            ret_relay_out(m).start()

    def stage_b(m):
        with jax.named_scope("y_wait"):
            y_copy(m).wait_recv()
        total = kept[lax.rem(m, LAG)] + y_in[m].astype(f32)

        pair = pair_at(m)

        @pl.when(pair // per == z)
        def _():
            acc[lax.rem(pair, per)] = total

        @pl.when(pair // per != z)
        def _():
            z_buf[m] = total.astype(bf16)
            z_copy(m, z, pair // per).start()

    def step(it):
        pl.when(it < steps)(lambda: begin(it))
        pl.when(jnp.logical_and(it >= 1, it <= steps))(lambda: stage_a(it - 1))
        if relayed:

            @pl.when(chip == 2)
            def _():
                pl.when(jnp.logical_and(it >= 2, it <= 6))(lambda: send_around(it - 2))
                pl.when(it == steps)(lambda: send_around(5))
                pl.when(it > steps)(lambda: every(2, lambda q: send_around(6 + q)))

            pl.when(it == steps)(lambda: every(2, lambda q: pass_return(q + 1)))
        pl.when(it == LAG)(lambda: every(LAG - 2, stage_b))
        pl.when(it >= LAG)(lambda: stage_b(it - 2))
        if relayed:
            pl.when(it == steps - 1)(lambda: every(3, corner_return))
            pl.when(it >= steps)(lambda: corner_return(it - 5))
            pl.when(it > steps)(lambda: pass_return(3))

        @pl.when(it < steps)
        def _():
            pltpu.make_async_copy(q_buf.at[it], q_buf.at[it], q_l.at[it]).wait()
            with jax.named_scope("attend"):
                attend(it)
            if relayed:
                pl.when(it == steps - 1)(lambda: pass_return(0))

    every(steps + 2, step)

    def finish(m):
        @pl.when(chip < chips - 1)
        def _():
            with jax.named_scope("ret_wait"):
                for a in range(2):
                    ret_copy(m, a).wait_recv()

        for a in range(2):
            for b, out in enumerate((dk_hbm, dv_hbm)):
                total = t0[m, a, b].astype(f32)
                total = total + jnp.where(par == 0, t1in[m, a, b].astype(f32), 0.0)
                total = total + jnp.where(chip < chips - 1, behind[m, a, b].astype(f32), 0.0)
                t0[m, a, b] = total.astype(bf16)
                dst = out.at[:, columns(pair_at(m) * PAIR + a * HEAD_DIM, HEAD_DIM)]
                pltpu.make_async_copy(t0.at[m, a, b], dst, out_s.at[m]).start()

    early = 3
    every(early, finish)
    if relayed:
        every(4, lambda q: pass_return(4 + q))
        corner_return(5)

    for s in range(1, nd):
        source = lax.rem(z + s, nd)
        for k in range(per):
            with jax.named_scope("z_wait"):
                z_arrive(source, k).wait_recv()
            acc[k] = acc[k] + z_in[source, k].astype(f32)
    base = jnp.int32(0)
    rows = span
    sent = []
    for level, b in enumerate(bits[1:]):
        rows //= 2
        up = lax.rem(i // b, 2)
        away = pl.ds(pl.multiple_of(base + (1 - up) * rows, rows), rows)
        base = base + up * rows
        stay = pl.ds(pl.multiple_of(base, rows), rows)
        at = pl.ds(span - 2 * rows, rows)
        for k in range(per):
            x_send[k, at, :] = acc[k, away, :].astype(bf16)
            sent.append(
                rdma(
                    x_send.at[k, at, :], x_in.at[k, at, :],
                    x_s.at[level * per + k], x_r.at[level * per + k], seq=flip(i, b),
                )
            )
            sent[-1].start()
        if level == 0:
            if relayed:
                every(2, lambda q: corner_return(q + 6))
            every(steps - 1 - early, lambda m: finish(m + early))
        for k in range(per):
            with jax.named_scope("x_wait"):
                sent[-per + k].wait_recv()
            acc[k, stay, :] = acc[k, stay, :] + x_in[k, at, :].astype(f32)
    mine = pl.ds(pl.multiple_of(base, own), own)
    for k in range(per):
        out_buf[k * PAIR : (k + 1) * PAIR, :] = acc[k, mine, :].T
    put = pltpu.make_async_copy(out_buf, wg_hbm, g_l.at[0])
    put.start()
    finish(steps - 1)

    def settle(m):
        for a in range(2):
            pl.when(chip < chips - 1)(lambda: far_copy(m, a).wait_send())
            pl.when(chip > 0)(lambda: ret_copy(m, a).wait_send())
            t1_copy(m, a).wait_send()
        if relayed:

            @pl.when(chip == 0)
            def _():
                ret_relay_out(m).wait_send()

            @pl.when(chip == chips - 1)
            def _():
                far_relay_out(m).wait_send()
                ret_relay2_out(m).wait_send()

        o_copy(m).wait_send()
        y_copy(m).wait_send()

        @pl.when(pair_at(m) // per != z)
        def _():
            z_copy(m, z, pair_at(m) // per).wait_send()
            w_mate(pair_at(m), par).wait_send()

        pl.when(jnp.logical_and(z < nd - 1, m < (z + 1) * per))(lambda: w_up(m).wait_send())
        pl.when(jnp.logical_and(z > 0, m >= z * per))(lambda: w_down(m).wait_send())
        pltpu.make_async_copy(dq_buf.at[m], dq_hbm.at[:, columns(pair_at(m) * PAIR, PAIR)], dq_s.at[m]).wait()
        pltpu.make_async_copy(t0.at[m], t0.at[m], out_s.at[m]).wait()

    with jax.named_scope("settle"):
        every(steps, settle)
    g_copy.wait_send()
    for copy in sent:
        copy.wait_send()
    put.wait()


def hand_over_kernel(*refs):
    count = len(refs) // 2
    for src, dst in zip(refs[:count], refs[count:]):
        dst[...] = src[...]


def hand_over(arrays, pieces):
    specs = [pl.BlockSpec((a.shape[0] // pieces, a.shape[1]), lambda p: (p, 0)) for a in arrays]
    return pl.pallas_call(
        hand_over_kernel,
        grid=(pieces,),
        in_specs=specs,
        out_specs=specs,
        out_shape=[jax.ShapeDtypeStruct(a.shape, a.dtype) for a in arrays],
        name="hand_over",
    )(*arrays)


def layer(n, nd, queries, keys, values, out_grad, proj_weight, lengths):
    f32, bf16 = jnp.float32, jnp.bfloat16
    tokens, feat = queries.shape[1:]
    rows, width = proj_weight.shape
    steps = feat // PAIR
    per = rows // PAIR
    half = width // 2
    span = half // 2
    own = width // n
    head = (steps, 2, tokens, HEAD_DIM)
    both = (steps, 2, 2, tokens, HEAD_DIM)
    pair = (steps, tokens, PAIR)
    levels = max(1, n.bit_length() - 3)
    vmem = [
        (head, bf16),
        *[(both, bf16)] * 6,
        *[((steps, 2, tokens, HEAD_DIM), bf16)] * 2,
        ((tokens, PAIR), bf16),
        *[(pair, bf16)] * 3,
        ((tokens, width), bf16),
        *[((half, tokens), bf16)] * 3,
        ((steps, 2, PAIR, half), bf16),
        *[((steps, span, PAIR), bf16)] * 3,
        ((nd, per, span, PAIR), bf16),
        ((LAG, span, PAIR), f32),
        ((per, span, PAIR), f32),
        *[((per, span, PAIR), bf16)] * 2,
        ((rows, own), f32),
    ]
    sems = [steps, steps, 1, 2 * per, steps, steps]
    sems += [2 * steps] * 8 + [steps] * 4
    sems += [steps, steps, 1, 1] + [steps] * 5 + [steps] * 3 + [nd * per] + [levels * per] * 2
    anywhere = pl.BlockSpec(memory_space=pl.ANY)
    grad = jax.ShapeDtypeStruct((tokens, feat), bf16)
    dq, dk, dv, wg = pl.pallas_call(
        functools.partial(kernel, n, nd),
        in_specs=[pl.BlockSpec(memory_space=pltpu.SMEM)] + [anywhere] * 5,
        out_specs=[anywhere] * 4,
        out_shape=[grad, grad, grad, jax.ShapeDtypeStruct((rows, own), f32)],
        scratch_shapes=[pltpu.VMEM(*spec) for spec in vmem] + [pltpu.SemaphoreType.DMA((s,)) for s in sems],
        compiler_params=pltpu.CompilerParams(
            collective_id=0, has_side_effects=True, vmem_limit_bytes=67043328
        ),
        name="banded_backward",
    )(lengths, queries[0], keys[0], values[0], out_grad[0], proj_weight)
    dq, dk, dv, wg = hand_over((dq, dk, dv, wg), 4)
    return dq[None], dk[None], dv[None], wg


def solution(mesh):
    rows = P("dp", "seq", None)
    return jax.shard_map(
        functools.partial(layer, mesh.shape["seq"], mesh.shape["dp"]),
        mesh=mesh,
        in_specs=(rows, rows, rows, rows, P("dp", None), P("dp")),
        out_specs=(rows, rows, rows, P("dp", "seq")),
        check_vma=False,
    )
```

```python
import functools

import jax
import jax.numpy as jnp
from jax import lax
from jax.experimental import pallas as pl
from jax.experimental.pallas import tpu as pltpu
from jax.sharding import PartitionSpec as P

HEAD_DIM = 128
PAIR = 2 * HEAD_DIM
LOG2E = 1.4426950408889634
NEG = -1e30
MESH = pl.DeviceIdType.MESH

NT = (((1,), (1,)), ((), ()))
NN = (((1,), (0,)), ((), ()))
TN = (((0,), (0,)), ((), ()))


def dot(a, b, dims):
    return lax.dot_general(a, b, dims, preferred_element_type=jnp.float32)


def flip(i, bit):
    return i + bit - 2 * bit * lax.rem(i // bit, 2)


def pair_order(count, per):
    orders = []
    for z in range(count):
        shards = sorted(range(count), key=lambda d: (abs(d - z), d < z))
        pairs = [d * per + k for d in shards for k in range(per)]
        if 0 < z < count - 1:
            pairs = pairs[:1] + pairs[per:] + pairs[1:per]
        orders.append(pairs)
    return orders


def pick(table, z, s):
    found = jnp.int32(0)
    for zz, row in enumerate(table):
        for ss, value in enumerate(row):
            found = found + jnp.where(z == zz, jnp.where(s == ss, value, 0), 0)
    return found


def every(count, body):
    def step(index, carry):
        body(index)
        return carry

    lax.fori_loop(0, count, step, 0)


def kernel(n, nd, len_ref, q_hbm, k_hbm, v_hbm, g_hbm, w_hbm, dq_hbm, dk_hbm, dv_hbm, wg_hbm, *scratch):
    (
        q_buf, kv, far, near, t0, t1in, behind, relay, relay2, do_buf, dq_buf, o_buf, o_in,
        g_buf, g_mine, g_send, g_in, g_side, g_pass, g_far, w_buf, o_side, o_far, y_send, y_in, z_buf, z_in, acc, x_send, x_in, out_buf,
        q_l, kv_l, g_l, w_l, dq_s, out_s,
        far_s, far_r, near_s, near_r, t1_s, t1_r, ret_s, ret_r, rel_s, rel_r, rel2_s, rel2_r,
        o_s, o_r, oa_s, oa_r, of_s, of_r, g_s, g_r, wu_s, wd_s, w_r, wp_s, wp_r, y_s, y_r, z_s, z_r, x_s, x_r,
    ) = scratch
    f32, bf16 = jnp.float32, jnp.bfloat16
    i, z = lax.axis_index("seq"), lax.axis_index("dp")
    steps, _, _, tokens, _ = kv.shape
    per = steps // nd
    chips = n // 2
    chip = i // 2
    par = lax.rem(i, 2)
    mate = flip(i, 1)
    ahead, back = lax.rem(i + 2, n), lax.rem(i + n - 2, n)
    across = flip(i, n // 2)
    beside = flip(i, 2)
    relayed = n == 8
    assert steps == 8
    width = w_hbm.shape[1]
    half = width // 2
    own = width // n
    span = half // 2
    table = pair_order(nd, per)

    def pair_at(it):
        return pick(table, z, it)

    def rdma(src, dst, send, recv, **where):
        return pltpu.make_async_remote_copy(
            src_ref=src, dst_ref=dst, send_sem=send, recv_sem=recv, device_id=where, device_id_type=MESH
        )

    def columns(start, size):
        return pl.ds(pl.multiple_of(start, 128), size)

    def load_kv(it):
        at = pair_at(it) * PAIR
        for a in range(2):
            for b, ref in enumerate((k_hbm, v_hbm)):
                src = ref.at[:, columns(at + a * HEAD_DIM, HEAD_DIM)]
                pltpu.make_async_copy(src, kv.at[it, a, b], kv_l.at[it]).start()

    def load_q(it):
        at = pair_at(it) * PAIR
        for a in range(2):
            src = q_hbm.at[:, columns(at + a * HEAD_DIM, HEAD_DIM)]
            pltpu.make_async_copy(src, q_buf.at[it, a], q_l.at[it]).start()

    bits = []
    bit = n // 2
    while bit > 1:
        bits.append(bit)
        bit //= 2
    greet = [dict(seq=mate), dict(seq=ahead), dict(seq=back)]
    greet += [dict(seq=flip(i, b)) for b in bits]
    greet += [dict(dp=lax.rem(z + s, nd)) for s in range(1, nd)]
    barrier = pltpu.get_barrier_semaphore()
    for who in greet:
        pl.semaphore_signal(barrier, inc=1, device_id=who, device_id_type=MESH)

    every(steps, load_kv)
    load_g = pltpu.make_async_copy(g_hbm, g_buf, g_l.at[0])
    load_g.start()
    own_w = []
    for k in range(per):
        for h in range(2):
            src = w_hbm.at[pl.ds(k * PAIR, PAIR), pl.ds(h * half, half)]
            own_w.append(pltpu.make_async_copy(src, w_buf.at[z * per + k, h], w_l.at[2 * k + h]))
            own_w[-1].start()
    every(steps, load_q)

    @pl.when(chip == 0)
    def _():
        def clear(it):
            far[it] = jnp.zeros_like(far[it])

        every(steps, clear)

    with jax.named_scope("greet"):
        pl.semaphore_wait(barrier, len(greet))

    def far_copy(it, a):
        return rdma(kv.at[it, a], far.at[it, a], far_s.at[2 * it + a], far_r.at[2 * it + a], seq=ahead)

    def far_relay_in(it):
        return rdma(kv.at[it, 1], relay.at[it], far_s.at[2 * it + 1], rel_r.at[it], seq=across)

    def far_relay_out(it):
        return rdma(relay.at[it], far.at[it, 1], rel_s.at[it], far_r.at[2 * it + 1], seq=beside)

    def ret_copy(it, a):
        return rdma(far.at[it, a], behind.at[it, a], ret_s.at[2 * it + a], ret_r.at[2 * it + a], seq=back)

    def ret_relay_in(it):
        return rdma(far.at[it, 1], relay.at[it], ret_s.at[2 * it + 1], rel_r.at[it], seq=across)

    def ret_relay_out(it):
        return rdma(relay.at[it], behind.at[it, 1], rel_s.at[it], ret_r.at[2 * it + 1], seq=beside)

    def ret_relay2_in(it):
        return rdma(far.at[it, 0], relay2.at[it], ret_s.at[2 * it], rel2_r.at[it], seq=beside)

    def ret_relay2_out(it):
        return rdma(relay2.at[it], behind.at[it, 0], rel2_s.at[it], ret_r.at[2 * it], seq=across)

    def near_copy(src, it, a):
        return rdma(src.at[it, a], near.at[it, a], near_s.at[2 * it + a], near_r.at[2 * it + a], seq=mate)

    def t1_copy(it, a):
        return rdma(near.at[it, a], t1in.at[it, a], t1_s.at[2 * it + a], t1_r.at[2 * it + a], seq=mate)

    def o_copy(it):
        return rdma(o_buf.at[it], o_in.at[it], o_s.at[it], o_r.at[it], seq=mate)

    def o_across(it):
        return rdma(o_buf.at[it], o_side.at[it], oa_s.at[it], oa_r.at[it], seq=across)

    def o_onward(it):
        return rdma(o_side.at[it], o_far.at[it], of_s.at[it], of_r.at[it], seq=mate)

    def y_copy(it):
        return rdma(y_send.at[it], y_in.at[it], y_s.at[it], y_r.at[it], seq=across)

    def w_up(piece):
        return rdma(w_buf.at[piece, par], w_buf.at[piece, par], wu_s.at[piece], w_r.at[piece], dp=lax.rem(z + 1, nd))

    def w_down(piece):
        return rdma(w_buf.at[piece, par], w_buf.at[piece, par], wd_s.at[piece], w_r.at[piece], dp=lax.rem(z + nd - 1, nd))

    def w_mate(piece, side):
        return rdma(w_buf.at[piece, side], w_buf.at[piece, side], wp_s.at[piece], wp_r.at[piece], seq=mate)

    def z_copy(it, source, shard):
        k = lax.rem(pair_at(it), per)
        return rdma(z_buf.at[it], z_in.at[source, k], z_s.at[it], z_r.at[source * per + k], dp=shard)

    def z_arrive(source, k):
        return rdma(z_buf.at[0], z_in.at[source, k], z_s.at[0], z_r.at[source * per + k], dp=source)

    def first_sends(it):
        with jax.named_scope("kv_load"):
            pltpu.make_async_copy(kv.at[it], kv.at[it], kv_l.at[it]).wait()

        @pl.when(chip < chips - 1)
        def _():
            far_copy(it, 0).start()
            if relayed:
                pl.when(chip != 1)(lambda: far_copy(it, 1).start())
                pl.when(chip == 1)(lambda: far_relay_in(it).start())
            else:
                far_copy(it, 1).start()

        @pl.when(par == 0)
        def _():
            for a in range(2):
                near_copy(kv, it, a).start()

    every(steps, first_sends)

    with jax.named_scope("w_load"):
        for copy in own_w:
            copy.wait()
    for k in range(per):
        pl.when(z < nd - 1)(lambda: w_up(z * per + k).start())
        pl.when(z > 0)(lambda: w_down(z * per + k).start())

    with jax.named_scope("g_load"):
        load_g.wait()
    at_row = i * tokens + lax.broadcasted_iota(jnp.int32, (tokens, 1), 0)
    live = at_row < len_ref[0]
    for c in range(chips):
        first = g_buf[:, 2 * c * own : (2 * c + 1) * own].astype(f32)
        second = g_buf[:, (2 * c + 1) * own : (2 * c + 2) * own].astype(f32)
        first, second = jnp.where(live, first, 0.0), jnp.where(live, second, 0.0)
        g_buf[:, 2 * c * own : (2 * c + 2) * own] = jnp.concatenate([first, second], 1).astype(bf16)
        g_mine[c * own : (c + 1) * own, :] = jnp.where(par == 0, first, second).T.astype(bf16)
        g_send[c * own : (c + 1) * own, :] = jnp.where(par == 0, second, first).T.astype(bf16)
    high = lax.rem(i // bits[0], 2)
    held = pl.ds(pl.multiple_of(high * span, span), span)
    given = pl.ds(pl.multiple_of((1 - high) * span, span), span)
    g_moves = [
        rdma(g_send, g_in, g_s.at[0], g_r.at[0], seq=mate),
        rdma(g_mine.at[given, :], g_side, g_s.at[1], g_r.at[1], seq=across),
        rdma(g_send.at[given, :], g_pass, g_s.at[2], g_r.at[2], seq=across),
    ]
    g_moves[0].start()

    @pl.when(high == 1)
    def _():
        for copy in g_moves[1:]:
            copy.start()

    g_moves.append(rdma(g_pass, g_far, g_s.at[3], g_r.at[3], seq=mate))

    def halo_relay(it):
        with jax.named_scope("hrel_wait"):
            far_relay_in(it).wait_recv()
        far_relay_out(it).start()

    if relayed:
        pl.when(chip == chips - 1)(lambda: halo_relay(0))

    scale = HEAD_DIM ** (-0.5)
    c_exp = scale * LOG2E

    def begin(it):
        @pl.when(chip > 0)
        def _():
            with jax.named_scope("far_wait"):
                for a in range(2):
                    far_copy(it, a).wait_recv()

        @pl.when(par == 1)
        def _():
            for a in range(2):
                near_copy(far, it, a).start()

        if relayed:
            for extra in range(2):
                at = 2 * it + extra

                @pl.when(jnp.logical_and(chip == chips - 1, jnp.logical_and(at > 0, at < steps)))
                def _():
                    halo_relay(at)

        piece = pair_at(it)

        @pl.when(piece // per != z)
        def _():
            with jax.named_scope("w_wait"):
                w_mate(piece, 1 - par).wait_recv()

        with jax.named_scope("do"):
            do = dot(g_buf[:, :half], w_buf[piece, 0], NT) + dot(g_buf[:, half:], w_buf[piece, 1], NT)
            do_buf[...] = do.astype(bf16)

    def give(m):
        with jax.named_scope("o_wait"):
            o_copy(m).wait_recv()

        @pl.when(high == 0)
        def _():
            with jax.named_scope("wgive"):
                part = dot(g_mine[given, :], o_buf[m], NN) + dot(g_in[given, :], o_in[m], NN)
                y_send[m] = part.astype(bf16)
            y_copy(m).start()

    def onward(m):
        @pl.when(high == 0)
        def _():
            with jax.named_scope("oa_wait"):
                o_across(m).wait_recv()
            o_onward(m).start()

    def combine(m):
        @pl.when(high == 0)
        def _():
            with jax.named_scope("of_wait"):
                o_onward(m).wait_recv()
            with jax.named_scope("wgrad"):
                total = dot(g_mine[held, :], o_buf[m], NN) + dot(g_in[held, :], o_in[m], NN)
                total = total + dot(g_side[...], o_side[m], NN) + dot(g_far[...], o_far[m], NN)
                place(m, total)

        @pl.when(high == 1)
        def _():
            with jax.named_scope("y_wait"):
                y_copy(m).wait_recv()
            with jax.named_scope("wgrad"):
                total = dot(g_mine[held, :], o_buf[m], NN) + dot(g_in[held, :], o_in[m], NN)
                place(m, total + y_in[m].astype(f32))

    def place(m, total):
        pair = pair_at(m)

        @pl.when(pair // per == z)
        def _():
            acc[lax.rem(pair, per)] = total

        @pl.when(pair // per != z)
        def _():
            z_buf[m] = total.astype(bf16)
            z_copy(m, z, pair // per).start()

    def pass_return(m):
        @pl.when(chip == chips - 1)
        def _():
            with jax.named_scope("rel2_wait"):
                ret_relay2_in(m).wait_recv()
            ret_relay2_out(m).start()

    def attend(it):
        causal_keys = lax.broadcasted_iota(jnp.int32, (tokens, tokens), 0)
        causal_queries = lax.broadcasted_iota(jnp.int32, (tokens, tokens), 1)
        for a in range(2):
            with jax.named_scope("near_wait"):
                near_copy(kv, it, a).wait_recv()
            q = q_buf[it, a]
            sources = (kv, near, far)
            parts, tops = [], []
            for offset, source in enumerate(sources):
                s = dot(source[it, a, 0], q, NT)
                if offset == 0:
                    s = jnp.where(causal_keys <= causal_queries, s, NEG)
                parts.append(s)
                top = jnp.max(s, axis=0, keepdims=True)
                if offset:
                    top = top + jnp.where(i >= offset, 0.0, NEG)
                tops.append(top)
            top = functools.reduce(jnp.maximum, tops) * c_exp
            total = None
            for offset in range(3):
                shift = top if offset == 0 else top + jnp.where(i >= offset, 0.0, -NEG)
                parts[offset] = jnp.exp2(parts[offset] * c_exp - shift)
                t = jnp.sum(parts[offset], axis=0, keepdims=True)
                total = t if total is None else total + t
            inverse = 1.0 / total
            out = None
            for offset, source in enumerate(sources):
                parts[offset] = parts[offset] * inverse
                o = dot(source[it, a, 1], parts[offset].astype(bf16), TN)
                out = o if out is None else out + o
            o = out.T.astype(bf16)
            o_buf[it, :, a * HEAD_DIM : (a + 1) * HEAD_DIM] = o
            do = do_buf[:, a * HEAD_DIM : (a + 1) * HEAD_DIM]
            delta = jnp.sum((do.astype(f32) * o.astype(f32)).T, axis=0, keepdims=True)
            near_copy(kv, it, a).wait_send()
            dq = None
            for offset, (source, term) in enumerate(zip(sources, (t0, near, far))):
                k, v = source[it, a, 0], source[it, a, 1]
                p = parts[offset]
                dv = dot(p.astype(bf16), do, NN)
                ds = (p * (dot(v, do, NT) - delta)).astype(bf16)
                dk = dot(ds, q, NN) * scale
                part = dot(k, ds, TN)
                dq = part if dq is None else dq + part
                term[it, a, 0] = dk.astype(bf16)
                term[it, a, 1] = dv.astype(bf16)
                if offset == 1:
                    t1_copy(it, a).start()
            dq_buf[it, :, a * HEAD_DIM : (a + 1) * HEAD_DIM] = (dq * scale).T.astype(bf16)
            if a == 0:
                pl.when(it < steps - 1)(lambda: move_weights(it))

                if relayed:
                    pl.when(it == steps - 1)(lambda: pass_return(0))

        o_copy(it).start()
        pl.when(high == 1)(lambda: o_across(it).start())
        pltpu.make_async_copy(dq_buf.at[it], dq_hbm.at[:, columns(pair_at(it) * PAIR, PAIR)], dq_s.at[it]).start()

    def move_weights(it):
        ends = jnp.logical_or(z == 0, z == nd - 1)
        j = it - jnp.where(ends, 1, 0)
        below, above = z - 1 - j // per, z + 1 + j // per

        @pl.when(jnp.logical_and(j >= 0, below >= 0))
        def _():
            piece = below * per + lax.rem(j, per)
            with jax.named_scope("up_wait"):
                w_up(piece).wait_recv()
            pl.when(z < nd - 1)(lambda: w_up(piece).start())
            w_mate(piece, par).start()

        @pl.when(jnp.logical_and(j >= 0, above <= nd - 1))
        def _():
            piece = above * per + lax.rem(j, per)
            with jax.named_scope("down_wait"):
                w_down(piece).wait_recv()
            pl.when(z > 0)(lambda: w_down(piece).start())
            w_mate(piece, par).start()

    def send_around(m):
        ret_relay2_in(m).start()
        ret_relay_in(m).start()

    def stage_a(m):
        for a in range(2):
            with jax.named_scope("t1_wait"):
                t1_copy(m, a).wait_recv()

            @pl.when(par == 1)
            def _():
                far[m, a] = (far[m, a].astype(f32) + t1in[m, a].astype(f32)).astype(bf16)

        @pl.when(chip > 0)
        def _():
            if relayed:

                @pl.when(chip != 2)
                def _():
                    ret_copy(m, 0).start()
                    ret_copy(m, 1).start()

                pl.when(jnp.logical_and(chip == 2, m < steps - 2))(lambda: send_around(m))

            else:
                ret_copy(m, 0).start()
                ret_copy(m, 1).start()

    def corner_return(m):
        @pl.when(chip == 0)
        def _():
            with jax.named_scope("rel_wait"):
                ret_relay_in(m).wait_recv()
            ret_relay_out(m).start()

    def stage_b(m):
        with jax.named_scope("y_wait"):
            y_copy(m).wait_recv()
        total = kept[lax.rem(m, LAG)] + y_in[m].astype(f32)

        pair = pair_at(m)

        @pl.when(pair // per == z)
        def _():
            acc[lax.rem(pair, per)] = total

        @pl.when(pair // per != z)
        def _():
            z_buf[m] = total.astype(bf16)
            z_copy(m, z, pair // per).start()

    def step(it):
        pl.when(it == 4)(lambda: every(3, onward))
        pl.when(it > 4)(lambda: onward(it - 2))
        begin(it)

        @pl.when(it >= 1)
        def _():
            stage_a(it - 1)
            pl.when(it == 1)(g_moves[0].wait_recv)
            give(it - 1)

        @pl.when(jnp.logical_and(it == 4, high == 0))
        def _():
            g_moves[2].wait_recv()
            g_moves[3].start()

        @pl.when(it == 5)
        def _():
            @pl.when(high == 0)
            def _():
                g_moves[1].wait_recv()
                g_moves[3].wait_recv()

            every(3, combine)

        pl.when(it > 4)(lambda: combine(it - 2))
        if relayed:
            pl.when(it == steps - 1)(lambda: every(4, corner_return))

        pltpu.make_async_copy(q_buf.at[it], q_buf.at[it], q_l.at[it]).wait()
        with jax.named_scope("attend"):
            attend(it)
        if relayed:
            pl.when(it == steps - 1)(lambda: pass_return(1))

    every(steps, step)
    first_left = steps - 2

    def trail(q):
        m = first_left + q
        onward(m)

        @pl.when(q == 0)
        def _():
            stage_a(steps - 1)
            give(steps - 1)

        if relayed:
            pl.when(jnp.logical_and(q == 0, chip == 2))(lambda: every(2, lambda r: send_around(steps - 2 + r)))
            pass_return(2 + q)
            corner_return(4 + q)
        combine(m)

    every(steps - first_left, trail)

    def finish(m):
        @pl.when(chip < chips - 1)
        def _():
            with jax.named_scope("ret_wait"):
                for a in range(2):
                    ret_copy(m, a).wait_recv()

        for a in range(2):
            for b, out in enumerate((dk_hbm, dv_hbm)):
                total = t0[m, a, b].astype(f32)
                total = total + jnp.where(par == 0, t1in[m, a, b].astype(f32), 0.0)
                total = total + jnp.where(chip < chips - 1, behind[m, a, b].astype(f32), 0.0)
                t0[m, a, b] = total.astype(bf16)
                dst = out.at[:, columns(pair_at(m) * PAIR + a * HEAD_DIM, HEAD_DIM)]
                pltpu.make_async_copy(t0.at[m, a, b], dst, out_s.at[m]).start()

    early = 3
    every(early, finish)
    if relayed:
        every(4, lambda q: pass_return(4 + q))
        every(2, lambda q: corner_return(6 + q))

    for s in range(1, nd):
        source = lax.rem(z + s, nd)
        for k in range(per):
            with jax.named_scope("z_wait"):
                z_arrive(source, k).wait_recv()
            acc[k] = acc[k] + z_in[source, k].astype(f32)
    base = jnp.int32(0)
    rows = span
    sent = []
    for level, b in enumerate(bits[1:]):
        rows //= 2
        up = lax.rem(i // b, 2)
        away = pl.ds(pl.multiple_of(base + (1 - up) * rows, rows), rows)
        base = base + up * rows
        stay = pl.ds(pl.multiple_of(base, rows), rows)
        at = pl.ds(span - 2 * rows, rows)
        for k in range(per):
            x_send[k, at, :] = acc[k, away, :].astype(bf16)
            sent.append(
                rdma(
                    x_send.at[k, at, :], x_in.at[k, at, :],
                    x_s.at[level * per + k], x_r.at[level * per + k], seq=flip(i, b),
                )
            )
            sent[-1].start()
        if level == 0:
            every(steps - 1 - early, lambda m: finish(m + early))
        for k in range(per):
            with jax.named_scope("x_wait"):
                sent[-per + k].wait_recv()
            acc[k, stay, :] = acc[k, stay, :] + x_in[k, at, :].astype(f32)
    mine = pl.ds(pl.multiple_of(base, own), own)
    for k in range(per):
        out_buf[k * PAIR : (k + 1) * PAIR, :] = acc[k, mine, :].T
    put = pltpu.make_async_copy(out_buf, wg_hbm, g_l.at[0])
    put.start()
    finish(steps - 1)

    def settle(m):
        for a in range(2):
            pl.when(chip < chips - 1)(lambda: far_copy(m, a).wait_send())
            pl.when(chip > 0)(lambda: ret_copy(m, a).wait_send())
            t1_copy(m, a).wait_send()
        if relayed:

            @pl.when(chip == 0)
            def _():
                ret_relay_out(m).wait_send()

            @pl.when(chip == chips - 1)
            def _():
                far_relay_out(m).wait_send()
                ret_relay2_out(m).wait_send()

        o_copy(m).wait_send()
        pl.when(high == 1)(lambda: o_across(m).wait_send())

        @pl.when(high == 0)
        def _():
            o_onward(m).wait_send()
            y_copy(m).wait_send()


        @pl.when(pair_at(m) // per != z)
        def _():
            z_copy(m, z, pair_at(m) // per).wait_send()
            w_mate(pair_at(m), par).wait_send()

        pl.when(jnp.logical_and(z < nd - 1, m < (z + 1) * per))(lambda: w_up(m).wait_send())
        pl.when(jnp.logical_and(z > 0, m >= z * per))(lambda: w_down(m).wait_send())
        pltpu.make_async_copy(dq_buf.at[m], dq_hbm.at[:, columns(pair_at(m) * PAIR, PAIR)], dq_s.at[m]).wait()
        pltpu.make_async_copy(t0.at[m], t0.at[m], out_s.at[m]).wait()

    with jax.named_scope("settle"):
        every(steps, settle)
    g_moves[0].wait_send()

    @pl.when(high == 1)
    def _():
        g_moves[1].wait_send()
        g_moves[2].wait_send()

    pl.when(high == 0)(g_moves[3].wait_send)
    for copy in sent:
        copy.wait_send()
    put.wait()


def hand_over_kernel(*refs):
    count = len(refs) // 2
    for src, dst in zip(refs[:count], refs[count:]):
        dst[...] = src[...]


def hand_over(arrays, pieces):
    specs = [pl.BlockSpec((a.shape[0] // pieces, a.shape[1]), lambda p: (p, 0)) for a in arrays]
    return pl.pallas_call(
        hand_over_kernel,
        grid=(pieces,),
        in_specs=specs,
        out_specs=specs,
        out_shape=[jax.ShapeDtypeStruct(a.shape, a.dtype) for a in arrays],
        name="hand_over",
    )(*arrays)


def layer(n, nd, queries, keys, values, out_grad, proj_weight, lengths):
    f32, bf16 = jnp.float32, jnp.bfloat16
    tokens, feat = queries.shape[1:]
    rows, width = proj_weight.shape
    steps = feat // PAIR
    per = rows // PAIR
    half = width // 2
    span = half // 2
    own = width // n
    head = (steps, 2, tokens, HEAD_DIM)
    both = (steps, 2, 2, tokens, HEAD_DIM)
    pair = (steps, tokens, PAIR)
    levels = max(1, n.bit_length() - 3)
    vmem = [
        (head, bf16),
        *[(both, bf16)] * 6,
        *[((steps, 2, tokens, HEAD_DIM), bf16)] * 2,
        ((tokens, PAIR), bf16),
        *[(pair, bf16)] * 3,
        ((tokens, width), bf16),
        *[((half, tokens), bf16)] * 3,
        *[((span, tokens), bf16)] * 3,
        ((steps, 2, PAIR, half), bf16),
        *[(pair, bf16)] * 2,
        *[((steps, span, PAIR), bf16)] * 3,
        ((nd, per, span, PAIR), bf16),
        ((per, span, PAIR), f32),
        *[((per, span, PAIR), bf16)] * 2,
        ((rows, own), f32),
    ]
    sems = [steps, steps, 1, 2 * per, steps, steps]
    sems += [2 * steps] * 8 + [steps] * 4
    sems += [steps] * 6 + [4, 4] + [steps] * 5 + [steps] * 3 + [nd * per] + [levels * per] * 2
    anywhere = pl.BlockSpec(memory_space=pl.ANY)
    grad = jax.ShapeDtypeStruct((tokens, feat), bf16)
    dq, dk, dv, wg = pl.pallas_call(
        functools.partial(kernel, n, nd),
        in_specs=[pl.BlockSpec(memory_space=pltpu.SMEM)] + [anywhere] * 5,
        out_specs=[anywhere] * 4,
        out_shape=[grad, grad, grad, jax.ShapeDtypeStruct((rows, own), f32)],
        scratch_shapes=[pltpu.VMEM(*spec) for spec in vmem] + [pltpu.SemaphoreType.DMA((s,)) for s in sems],
        compiler_params=pltpu.CompilerParams(
            collective_id=0, has_side_effects=True, vmem_limit_bytes=67043328
        ),
        name="banded_backward",
    )(lengths, queries[0], keys[0], values[0], out_grad[0], proj_weight)
    dq, dk, dv, wg = hand_over((dq, dk, dv, wg), 2)
    return dq[None], dk[None], dv[None], wg


def solution(mesh):
    rows = P("dp", "seq", None)
    return jax.shard_map(
        functools.partial(layer, mesh.shape["seq"], mesh.shape["dp"]),
        mesh=mesh,
        in_specs=(rows, rows, rows, rows, P("dp", None), P("dp")),
        out_specs=(rows, rows, rows, P("dp", "seq")),
        check_vma=False,
    )
```

```python
import functools

import jax
import jax.numpy as jnp
from jax import lax
from jax.experimental import pallas as pl
from jax.experimental.pallas import tpu as pltpu
from jax.sharding import PartitionSpec as P

HEAD_DIM = 128
PAIR = 2 * HEAD_DIM
LOG2E = 1.4426950408889634
NEG = -1e30
MESH = pl.DeviceIdType.MESH

NT = (((1,), (1,)), ((), ()))
NN = (((1,), (0,)), ((), ()))
TN = (((0,), (0,)), ((), ()))


def dot(a, b, dims):
    return lax.dot_general(a, b, dims, preferred_element_type=jnp.float32)


def flip(i, bit):
    return i + bit - 2 * bit * lax.rem(i // bit, 2)


def pair_order(count, per):
    orders = []
    for z in range(count):
        shards = sorted(range(count), key=lambda d: (abs(d - z), d < z))
        pairs = [d * per + k for d in shards for k in range(per)]
        if 0 < z < count - 1:
            pairs = pairs[:1] + pairs[per:] + pairs[1:per]
        orders.append(pairs)
    return orders


def pick(table, z, s):
    found = jnp.int32(0)
    for zz, row in enumerate(table):
        for ss, value in enumerate(row):
            found = found + jnp.where(z == zz, jnp.where(s == ss, value, 0), 0)
    return found


def every(count, body):
    def step(index, carry):
        body(index)
        return carry

    lax.fori_loop(0, count, step, 0)


def kernel(n, nd, len_ref, q_hbm, k_hbm, v_hbm, g_hbm, w_hbm, dq_hbm, dk_hbm, dv_hbm, wg_hbm, *scratch):
    (
        q_buf, kv, far, near, t0, t1in, behind, relay, relay2, do_buf, dq_buf, o_buf, o_in,
        g_buf, g_mine, g_send, g_in, g_side, g_pass, g_far, w_buf, o_side, o_far, y_send, y_in, z_buf, z_in, acc, x_send, x_in, out_buf,
        q_l, kv_l, g_l, w_l, dq_s, out_s,
        far_s, far_r, near_s, near_r, t1_s, t1_r, ret_s, ret_r, rel_s, rel_r, rel2_s, rel2_r,
        o_s, o_r, oa_s, oa_r, of_s, of_r, g_s, g_r, wu_s, wd_s, w_r, wp_s, wp_r, y_s, y_r, z_s, z_r, x_s, x_r,
    ) = scratch
    f32, bf16 = jnp.float32, jnp.bfloat16
    i, z = lax.axis_index("seq"), lax.axis_index("dp")
    steps, _, _, tokens, _ = kv.shape
    per = steps // nd
    chips = n // 2
    chip = i // 2
    par = lax.rem(i, 2)
    mate = flip(i, 1)
    ahead, back = lax.rem(i + 2, n), lax.rem(i + n - 2, n)
    across = flip(i, n // 2)
    beside = flip(i, 2)
    relayed = n == 8
    assert steps == 8
    width = w_hbm.shape[1]
    half = width // 2
    own = width // n
    span = half // 2
    table = pair_order(nd, per)

    def pair_at(it):
        return pick(table, z, it)

    def rdma(src, dst, send, recv, **where):
        return pltpu.make_async_remote_copy(
            src_ref=src, dst_ref=dst, send_sem=send, recv_sem=recv, device_id=where, device_id_type=MESH
        )

    def columns(start, size):
        return pl.ds(pl.multiple_of(start, 128), size)

    def load_kv(it):
        at = pair_at(it) * PAIR
        for a in range(2):
            for b, ref in enumerate((k_hbm, v_hbm)):
                src = ref.at[:, columns(at + a * HEAD_DIM, HEAD_DIM)]
                pltpu.make_async_copy(src, kv.at[it, a, b], kv_l.at[it]).start()

    def load_q(it):
        at = pair_at(it) * PAIR
        for a in range(2):
            src = q_hbm.at[:, columns(at + a * HEAD_DIM, HEAD_DIM)]
            pltpu.make_async_copy(src, q_buf.at[it, a], q_l.at[it]).start()

    bits = []
    bit = n // 2
    while bit > 1:
        bits.append(bit)
        bit //= 2
    greet = [dict(seq=mate), dict(seq=ahead), dict(seq=back)]
    greet += [dict(seq=flip(i, b)) for b in bits]
    greet += [dict(dp=lax.rem(z + s, nd)) for s in range(1, nd)]
    barrier = pltpu.get_barrier_semaphore()
    for who in greet:
        pl.semaphore_signal(barrier, inc=1, device_id=who, device_id_type=MESH)

    every(steps, load_kv)
    load_g = pltpu.make_async_copy(g_hbm, g_buf, g_l.at[0])
    load_g.start()
    own_w = []
    for k in range(per):
        for h in range(2):
            src = w_hbm.at[pl.ds(k * PAIR, PAIR), pl.ds(h * half, half)]
            own_w.append(pltpu.make_async_copy(src, w_buf.at[z * per + k, h], w_l.at[2 * k + h]))
            own_w[-1].start()
    every(steps, load_q)

    @pl.when(chip == 0)
    def _():
        def clear(it):
            far[it] = jnp.zeros_like(far[it])

        every(steps, clear)

    with jax.named_scope("greet"):
        pl.semaphore_wait(barrier, len(greet))

    def far_copy(it, a):
        return rdma(kv.at[it, a], far.at[it, a], far_s.at[2 * it + a], far_r.at[2 * it + a], seq=ahead)

    def far_relay_in(it):
        return rdma(kv.at[it, 1], relay.at[it], far_s.at[2 * it + 1], rel_r.at[it], seq=across)

    def far_relay_out(it):
        return rdma(relay.at[it], far.at[it, 1], rel_s.at[it], far_r.at[2 * it + 1], seq=beside)

    def ret_copy(it, a):
        return rdma(far.at[it, a], behind.at[it, a], ret_s.at[2 * it + a], ret_r.at[2 * it + a], seq=back)

    def ret_relay_in(it):
        return rdma(far.at[it, 1], relay.at[it], ret_s.at[2 * it + 1], rel_r.at[it], seq=across)

    def ret_relay_out(it):
        return rdma(relay.at[it], behind.at[it, 1], rel_s.at[it], ret_r.at[2 * it + 1], seq=beside)

    def ret_relay2_in(it):
        return rdma(far.at[it, 0], relay2.at[it], ret_s.at[2 * it], rel2_r.at[it], seq=beside)

    def ret_relay2_out(it):
        return rdma(relay2.at[it], behind.at[it, 0], rel2_s.at[it], ret_r.at[2 * it], seq=across)

    def shift_in(it):
        return rdma(far.at[it, 0], relay2.at[it], ret_s.at[2 * it], rel2_r.at[it], seq=across)

    def shift_out(it):
        return rdma(relay2.at[it], behind.at[it, 0], rel2_s.at[it], ret_r.at[2 * it], seq=beside)

    def near_copy(src, it, a):
        return rdma(src.at[it, a], near.at[it, a], near_s.at[2 * it + a], near_r.at[2 * it + a], seq=mate)

    def t1_copy(it, a):
        return rdma(near.at[it, a], t1in.at[it, a], t1_s.at[2 * it + a], t1_r.at[2 * it + a], seq=mate)

    def o_copy(it):
        return rdma(o_buf.at[it], o_in.at[it], o_s.at[it], o_r.at[it], seq=mate)

    def o_across(it):
        return rdma(o_buf.at[it], o_side.at[it], oa_s.at[it], oa_r.at[it], seq=across)

    def o_onward(it):
        return rdma(o_side.at[it], o_far.at[it], of_s.at[it], of_r.at[it], seq=mate)

    def y_copy(it):
        return rdma(y_send.at[it], y_in.at[it], y_s.at[it], y_r.at[it], seq=across)

    def w_up(piece):
        return rdma(w_buf.at[piece, par], w_buf.at[piece, par], wu_s.at[piece], w_r.at[piece], dp=lax.rem(z + 1, nd))

    def w_down(piece):
        return rdma(w_buf.at[piece, par], w_buf.at[piece, par], wd_s.at[piece], w_r.at[piece], dp=lax.rem(z + nd - 1, nd))

    def w_mate(piece, side):
        return rdma(w_buf.at[piece, side], w_buf.at[piece, side], wp_s.at[piece], wp_r.at[piece], seq=mate)

    def z_copy(it, source, shard):
        k = lax.rem(pair_at(it), per)
        return rdma(z_buf.at[it], z_in.at[source, k], z_s.at[it], z_r.at[source * per + k], dp=shard)

    def z_arrive(source, k):
        return rdma(z_buf.at[0], z_in.at[source, k], z_s.at[0], z_r.at[source * per + k], dp=source)

    def first_sends(it):
        with jax.named_scope("kv_load"):
            pltpu.make_async_copy(kv.at[it], kv.at[it], kv_l.at[it]).wait()

        @pl.when(chip < chips - 1)
        def _():
            far_copy(it, 0).start()
            if relayed:
                pl.when(chip != 1)(lambda: far_copy(it, 1).start())
                pl.when(chip == 1)(lambda: far_relay_in(it).start())
            else:
                far_copy(it, 1).start()

        @pl.when(par == 0)
        def _():
            for a in range(2):
                near_copy(kv, it, a).start()

    every(steps, first_sends)

    with jax.named_scope("w_load"):
        for copy in own_w:
            copy.wait()
    for k in range(per):
        pl.when(z < nd - 1)(lambda: w_up(z * per + k).start())
        pl.when(z > 0)(lambda: w_down(z * per + k).start())

    with jax.named_scope("g_load"):
        load_g.wait()
    at_row = i * tokens + lax.broadcasted_iota(jnp.int32, (tokens, 1), 0)
    live = at_row < len_ref[0]
    for c in range(chips):
        first = g_buf[:, 2 * c * own : (2 * c + 1) * own].astype(f32)
        second = g_buf[:, (2 * c + 1) * own : (2 * c + 2) * own].astype(f32)
        first, second = jnp.where(live, first, 0.0), jnp.where(live, second, 0.0)
        g_buf[:, 2 * c * own : (2 * c + 2) * own] = jnp.concatenate([first, second], 1).astype(bf16)
        g_mine[c * own : (c + 1) * own, :] = jnp.where(par == 0, first, second).T.astype(bf16)
        g_send[c * own : (c + 1) * own, :] = jnp.where(par == 0, second, first).T.astype(bf16)
    high = lax.rem(i // bits[0], 2)
    held = pl.ds(pl.multiple_of(high * span, span), span)
    given = pl.ds(pl.multiple_of((1 - high) * span, span), span)
    g_moves = [
        rdma(g_send, g_in, g_s.at[0], g_r.at[0], seq=mate),
        rdma(g_mine.at[given, :], g_side, g_s.at[1], g_r.at[1], seq=across),
        rdma(g_send.at[given, :], g_pass, g_s.at[2], g_r.at[2], seq=across),
    ]
    g_moves[0].start()

    @pl.when(high == 1)
    def _():
        for copy in g_moves[1:]:
            copy.start()

    g_moves.append(rdma(g_pass, g_far, g_s.at[3], g_r.at[3], seq=mate))

    def halo_relay(it):
        with jax.named_scope("hrel_wait"):
            far_relay_in(it).wait_recv()
        far_relay_out(it).start()

    if relayed:
        pl.when(chip == chips - 1)(lambda: halo_relay(0))

    scale = HEAD_DIM ** (-0.5)
    c_exp = scale * LOG2E

    def begin(it):
        @pl.when(chip > 0)
        def _():
            with jax.named_scope("far_wait"):
                for a in range(2):
                    far_copy(it, a).wait_recv()

        @pl.when(par == 1)
        def _():
            for a in range(2):
                near_copy(far, it, a).start()

        if relayed:
            for extra in range(2):
                at = 2 * it + extra

                @pl.when(jnp.logical_and(chip == chips - 1, jnp.logical_and(at > 0, at < steps)))
                def _():
                    halo_relay(at)

        piece = pair_at(it)

        @pl.when(piece // per != z)
        def _():
            with jax.named_scope("w_wait"):
                w_mate(piece, 1 - par).wait_recv()

        with jax.named_scope("do"):
            do = dot(g_buf[:, :half], w_buf[piece, 0], NT) + dot(g_buf[:, half:], w_buf[piece, 1], NT)
            do_buf[...] = do.astype(bf16)

    def give(m):
        with jax.named_scope("o_wait"):
            o_copy(m).wait_recv()

        @pl.when(high == 0)
        def _():
            with jax.named_scope("wgive"):
                part = dot(g_mine[given, :], o_buf[m], NN) + dot(g_in[given, :], o_in[m], NN)
                y_send[m] = part.astype(bf16)
            y_copy(m).start()

    def onward(m):
        @pl.when(high == 0)
        def _():
            with jax.named_scope("oa_wait"):
                o_across(m).wait_recv()
            o_onward(m).start()

    def combine(m):
        @pl.when(high == 0)
        def _():
            with jax.named_scope("of_wait"):
                o_onward(m).wait_recv()
            with jax.named_scope("wgrad"):
                total = dot(g_mine[held, :], o_buf[m], NN) + dot(g_in[held, :], o_in[m], NN)
                total = total + dot(g_side[...], o_side[m], NN) + dot(g_far[...], o_far[m], NN)
                place(m, total)

        @pl.when(high == 1)
        def _():
            with jax.named_scope("y_wait"):
                y_copy(m).wait_recv()
            with jax.named_scope("wgrad"):
                total = dot(g_mine[held, :], o_buf[m], NN) + dot(g_in[held, :], o_in[m], NN)
                place(m, total + y_in[m].astype(f32))

    def place(m, total):
        pair = pair_at(m)

        @pl.when(pair // per == z)
        def _():
            acc[lax.rem(pair, per)] = total

        @pl.when(pair // per != z)
        def _():
            z_buf[m] = total.astype(bf16)
            z_copy(m, z, pair // per).start()

    def pass_return(m):
        @pl.when(chip == chips - 1)
        def _():
            with jax.named_scope("rel2_wait"):
                ret_relay2_in(m).wait_recv()
            ret_relay2_out(m).start()

    def attend(it):
        causal_keys = lax.broadcasted_iota(jnp.int32, (tokens, tokens), 0)
        causal_queries = lax.broadcasted_iota(jnp.int32, (tokens, tokens), 1)
        for a in range(2):
            with jax.named_scope("near_wait"):
                near_copy(kv, it, a).wait_recv()
            q = q_buf[it, a]
            sources = (kv, near, far)
            parts, tops = [], []
            for offset, source in enumerate(sources):
                s = dot(source[it, a, 0], q, NT)
                if offset == 0:
                    s = jnp.where(causal_keys <= causal_queries, s, NEG)
                parts.append(s)
                top = jnp.max(s, axis=0, keepdims=True)
                if offset:
                    top = top + jnp.where(i >= offset, 0.0, NEG)
                tops.append(top)
            top = functools.reduce(jnp.maximum, tops) * c_exp
            total = None
            for offset in range(3):
                shift = top if offset == 0 else top + jnp.where(i >= offset, 0.0, -NEG)
                parts[offset] = jnp.exp2(parts[offset] * c_exp - shift)
                t = jnp.sum(parts[offset], axis=0, keepdims=True)
                total = t if total is None else total + t
            inverse = 1.0 / total
            out = None
            for offset, source in enumerate(sources):
                parts[offset] = parts[offset] * inverse
                o = dot(source[it, a, 1], parts[offset].astype(bf16), TN)
                out = o if out is None else out + o
            o = out.T.astype(bf16)
            o_buf[it, :, a * HEAD_DIM : (a + 1) * HEAD_DIM] = o
            do = do_buf[:, a * HEAD_DIM : (a + 1) * HEAD_DIM]
            delta = jnp.sum((do.astype(f32) * o.astype(f32)).T, axis=0, keepdims=True)
            near_copy(kv, it, a).wait_send()
            dq = None
            for offset, (source, term) in enumerate(zip(sources, (t0, near, far))):
                k, v = source[it, a, 0], source[it, a, 1]
                p = parts[offset]
                dv = dot(p.astype(bf16), do, NN)
                ds = (p * (dot(v, do, NT) - delta)).astype(bf16)
                dk = dot(ds, q, NN) * scale
                part = dot(k, ds, TN)
                dq = part if dq is None else dq + part
                term[it, a, 0] = dk.astype(bf16)
                term[it, a, 1] = dv.astype(bf16)
                if offset == 1:
                    t1_copy(it, a).start()
            dq_buf[it, :, a * HEAD_DIM : (a + 1) * HEAD_DIM] = (dq * scale).T.astype(bf16)
            if a == 0:
                pl.when(it < steps - 1)(lambda: move_weights(it))

                if relayed:
                    pl.when(it == steps - 1)(lambda: pass_return(0))

        o_copy(it).start()
        pl.when(high == 1)(lambda: o_across(it).start())
        pltpu.make_async_copy(dq_buf.at[it], dq_hbm.at[:, columns(pair_at(it) * PAIR, PAIR)], dq_s.at[it]).start()

    def move_weights(it):
        ends = jnp.logical_or(z == 0, z == nd - 1)
        j = it - jnp.where(ends, 1, 0)
        below, above = z - 1 - j // per, z + 1 + j // per

        @pl.when(jnp.logical_and(j >= 0, below >= 0))
        def _():
            piece = below * per + lax.rem(j, per)
            with jax.named_scope("up_wait"):
                w_up(piece).wait_recv()
            pl.when(z < nd - 1)(lambda: w_up(piece).start())
            w_mate(piece, par).start()

        @pl.when(jnp.logical_and(j >= 0, above <= nd - 1))
        def _():
            piece = above * per + lax.rem(j, per)
            with jax.named_scope("down_wait"):
                w_down(piece).wait_recv()
            pl.when(z > 0)(lambda: w_down(piece).start())
            w_mate(piece, par).start()

    def send_around(m):
        pl.when(m < steps - 1)(lambda: ret_relay2_in(m).start())
        ret_relay_in(m).start()
        pl.when(m == steps - 1)(lambda: shift_in(m).start())

    def stage_a(m):
        for a in range(2):
            with jax.named_scope("t1_wait"):
                t1_copy(m, a).wait_recv()

            @pl.when(par == 1)
            def _():
                far[m, a] = (far[m, a].astype(f32) + t1in[m, a].astype(f32)).astype(bf16)

        @pl.when(chip > 0)
        def _():
            if relayed:

                @pl.when(chip != 2)
                def _():
                    ret_copy(m, 0).start()
                    ret_copy(m, 1).start()

                pl.when(jnp.logical_and(chip == 2, m < steps - 2))(lambda: send_around(m))

            else:
                ret_copy(m, 0).start()
                ret_copy(m, 1).start()

    def corner_return(m):
        @pl.when(chip == 0)
        def _():
            with jax.named_scope("rel_wait"):
                ret_relay_in(m).wait_recv()
            ret_relay_out(m).start()

            @pl.when(jnp.int32(m) == steps - 1)
            def _():
                shift_in(m).wait_recv()
                shift_out(m).start()

    def step(it):
        pl.when(it == 4)(lambda: every(3, onward))
        pl.when(it > 4)(lambda: onward(it - 2))
        begin(it)

        @pl.when(it >= 1)
        def _():
            stage_a(it - 1)
            pl.when(it == 1)(g_moves[0].wait_recv)
            give(it - 1)

        @pl.when(jnp.logical_and(it == 4, high == 0))
        def _():
            g_moves[2].wait_recv()
            g_moves[3].start()

        @pl.when(it == 5)
        def _():
            @pl.when(high == 0)
            def _():
                g_moves[1].wait_recv()
                g_moves[3].wait_recv()

            every(3, combine)

        pl.when(it > 4)(lambda: combine(it - 2))
        if relayed:
            pl.when(it == steps - 2)(lambda: every(4, corner_return))
            pl.when(it == steps - 1)(lambda: corner_return(4))

        pltpu.make_async_copy(q_buf.at[it], q_buf.at[it], q_l.at[it]).wait()
        with jax.named_scope("attend"):
            attend(it)
        if relayed:
            pl.when(it == steps - 1)(lambda: pass_return(1))

    every(steps, step)
    first_left = steps - 2

    def trail(q):
        m = first_left + q
        onward(m)

        @pl.when(q == 0)
        def _():
            stage_a(steps - 1)
            give(steps - 1)

        if relayed:
            pl.when(jnp.logical_and(q == 0, chip == 2))(lambda: every(2, lambda r: send_around(steps - 2 + r)))
            pass_return(2 + q)
            pl.when(q == 0)(lambda: corner_return(5))
        combine(m)

    every(steps - first_left, trail)

    def finish(m):
        @pl.when(chip < chips - 1)
        def _():
            with jax.named_scope("ret_wait"):
                for a in range(2):
                    ret_copy(m, a).wait_recv()

        for a in range(2):
            for b, out in enumerate((dk_hbm, dv_hbm)):
                total = t0[m, a, b].astype(f32)
                total = total + jnp.where(par == 0, t1in[m, a, b].astype(f32), 0.0)
                total = total + jnp.where(chip < chips - 1, behind[m, a, b].astype(f32), 0.0)
                t0[m, a, b] = total.astype(bf16)
                dst = out.at[:, columns(pair_at(m) * PAIR + a * HEAD_DIM, HEAD_DIM)]
                pltpu.make_async_copy(t0.at[m, a, b], dst, out_s.at[m]).start()

    early = 3
    every(early, finish)
    if relayed:
        every(3, lambda q: pass_return(4 + q))
        every(2, lambda q: corner_return(6 + q))

    base = jnp.int32(0)
    rows = span
    levels = []
    for b in bits[1:]:
        rows //= 2
        up = lax.rem(i // b, 2)
        away = pl.ds(pl.multiple_of(base + (1 - up) * rows, rows), rows)
        base = base + up * rows
        levels.append((b, away, pl.ds(pl.multiple_of(base, rows), rows), pl.ds(span - 2 * rows, rows)))

    def x_copy(level, k):
        b, _, _, at = levels[level]
        sems = (x_s.at[level * per + k], x_r.at[level * per + k])
        return rdma(x_send.at[k, at, :], x_in.at[k, at, :], *sems, seq=flip(i, b))

    def x_start(level, k):
        _, away, _, at = levels[level]
        x_send[k, at, :] = acc[k, away, :].astype(bf16)
        x_copy(level, k).start()

    def x_finish(level, k):
        _, _, stay, at = levels[level]
        with jax.named_scope("x_wait"):
            x_copy(level, k).wait_recv()
        acc[k, stay, :] = acc[k, stay, :] + x_in[k, at, :].astype(f32)

    for k in range(per):
        for s in range(1, nd):
            source = lax.rem(z + s, nd)
            with jax.named_scope("z_wait"):
                z_arrive(source, k).wait_recv()
            acc[k] = acc[k] + z_in[source, k].astype(f32)
        if levels:
            x_start(0, k)
    every(steps - 1 - early, lambda m: finish(m + early))
    for level in range(len(levels)):
        for k in range(per):
            if level:
                x_start(level, k)
        for k in range(per):
            x_finish(level, k)
    mine = pl.ds(pl.multiple_of(base, own), own)
    for k in range(per):
        out_buf[k * PAIR : (k + 1) * PAIR, :] = acc[k, mine, :].T
    put = pltpu.make_async_copy(out_buf, wg_hbm, g_l.at[0])
    put.start()
    finish(steps - 1)

    def settle(m):
        for a in range(2):
            pl.when(chip < chips - 1)(lambda: far_copy(m, a).wait_send())
            pl.when(chip > 0)(lambda: ret_copy(m, a).wait_send())
            t1_copy(m, a).wait_send()
        if relayed:

            @pl.when(chip == 0)
            def _():
                ret_relay_out(m).wait_send()
                pl.when(m == steps - 1)(lambda: shift_out(m).wait_send())

            @pl.when(chip == chips - 1)
            def _():
                far_relay_out(m).wait_send()
                pl.when(m < steps - 1)(lambda: ret_relay2_out(m).wait_send())

        o_copy(m).wait_send()
        pl.when(high == 1)(lambda: o_across(m).wait_send())

        @pl.when(high == 0)
        def _():
            o_onward(m).wait_send()
            y_copy(m).wait_send()


        @pl.when(pair_at(m) // per != z)
        def _():
            z_copy(m, z, pair_at(m) // per).wait_send()
            w_mate(pair_at(m), par).wait_send()

        pl.when(jnp.logical_and(z < nd - 1, m < (z + 1) * per))(lambda: w_up(m).wait_send())
        pl.when(jnp.logical_and(z > 0, m >= z * per))(lambda: w_down(m).wait_send())
        pltpu.make_async_copy(dq_buf.at[m], dq_hbm.at[:, columns(pair_at(m) * PAIR, PAIR)], dq_s.at[m]).wait()
        pltpu.make_async_copy(t0.at[m], t0.at[m], out_s.at[m]).wait()

    with jax.named_scope("settle"):
        every(steps, settle)
    g_moves[0].wait_send()

    @pl.when(high == 1)
    def _():
        g_moves[1].wait_send()
        g_moves[2].wait_send()

    pl.when(high == 0)(g_moves[3].wait_send)
    for level in range(len(levels)):
        for k in range(per):
            x_copy(level, k).wait_send()
    put.wait()


def hand_over_kernel(*refs):
    count = len(refs) // 2
    for src, dst in zip(refs[:count], refs[count:]):
        dst[...] = src[...]


def hand_over(arrays, pieces):
    specs = [pl.BlockSpec((a.shape[0] // pieces, a.shape[1]), lambda p: (p, 0)) for a in arrays]
    return pl.pallas_call(
        hand_over_kernel,
        grid=(pieces,),
        in_specs=specs,
        out_specs=specs,
        out_shape=[jax.ShapeDtypeStruct(a.shape, a.dtype) for a in arrays],
        name="hand_over",
    )(*arrays)


def layer(n, nd, queries, keys, values, out_grad, proj_weight, lengths):
    f32, bf16 = jnp.float32, jnp.bfloat16
    tokens, feat = queries.shape[1:]
    rows, width = proj_weight.shape
    steps = feat // PAIR
    per = rows // PAIR
    half = width // 2
    span = half // 2
    own = width // n
    head = (steps, 2, tokens, HEAD_DIM)
    both = (steps, 2, 2, tokens, HEAD_DIM)
    pair = (steps, tokens, PAIR)
    levels = max(1, n.bit_length() - 3)
    vmem = [
        (head, bf16),
        *[(both, bf16)] * 6,
        *[((steps, 2, tokens, HEAD_DIM), bf16)] * 2,
        ((tokens, PAIR), bf16),
        *[(pair, bf16)] * 3,
        ((tokens, width), bf16),
        *[((half, tokens), bf16)] * 3,
        *[((span, tokens), bf16)] * 3,
        ((steps, 2, PAIR, half), bf16),
        *[(pair, bf16)] * 2,
        *[((steps, span, PAIR), bf16)] * 3,
        ((nd, per, span, PAIR), bf16),
        ((per, span, PAIR), f32),
        *[((per, span, PAIR), bf16)] * 2,
        ((rows, own), f32),
    ]
    sems = [steps, steps, 1, 2 * per, steps, steps]
    sems += [2 * steps] * 8 + [steps] * 4
    sems += [steps] * 6 + [4, 4] + [steps] * 5 + [steps] * 3 + [nd * per] + [levels * per] * 2
    anywhere = pl.BlockSpec(memory_space=pl.ANY)
    grad = jax.ShapeDtypeStruct((tokens, feat), bf16)
    dq, dk, dv, wg = pl.pallas_call(
        functools.partial(kernel, n, nd),
        in_specs=[pl.BlockSpec(memory_space=pltpu.SMEM)] + [anywhere] * 5,
        out_specs=[anywhere] * 4,
        out_shape=[grad, grad, grad, jax.ShapeDtypeStruct((rows, own), f32)],
        scratch_shapes=[pltpu.VMEM(*spec) for spec in vmem] + [pltpu.SemaphoreType.DMA((s,)) for s in sems],
        compiler_params=pltpu.CompilerParams(
            collective_id=0, has_side_effects=True, vmem_limit_bytes=67043328
        ),
        name="banded_backward",
    )(lengths, queries[0], keys[0], values[0], out_grad[0], proj_weight)
    dq, dk, dv, wg = hand_over((dq, dk, dv, wg), 2)
    return dq[None], dk[None], dv[None], wg


def solution(mesh):
    rows = P("dp", "seq", None)
    return jax.shard_map(
        functools.partial(layer, mesh.shape["seq"], mesh.shape["dp"]),
        mesh=mesh,
        in_specs=(rows, rows, rows, rows, P("dp", None), P("dp")),
        out_specs=(rows, rows, rows, P("dp", "seq")),
        check_vma=False,
    )
```

```python
import functools

import jax
import jax.numpy as jnp
from jax import lax
from jax.experimental import pallas as pl
from jax.experimental.pallas import tpu as pltpu
from jax.sharding import PartitionSpec as P

HEAD_DIM = 128
PAIR = 2 * HEAD_DIM
LOG2E = 1.4426950408889634
NEG = -1e30
MESH = pl.DeviceIdType.MESH

NT = (((1,), (1,)), ((), ()))
NN = (((1,), (0,)), ((), ()))
TN = (((0,), (0,)), ((), ()))


def dot(a, b, dims):
    return lax.dot_general(a, b, dims, preferred_element_type=jnp.float32)


def flip(i, bit):
    return i + bit - 2 * bit * lax.rem(i // bit, 2)


def pair_order(count, per):
    orders = []
    for z in range(count):
        shards = sorted(range(count), key=lambda d: (abs(d - z), d < z))
        pairs = [d * per + k for d in shards for k in range(per)]
        if 0 < z < count - 1:
            pairs = pairs[:1] + pairs[per:] + pairs[1:per]
        orders.append(pairs)
    return orders


def pick(table, z, s):
    found = jnp.int32(0)
    for zz, row in enumerate(table):
        for ss, value in enumerate(row):
            found = found + jnp.where(z == zz, jnp.where(s == ss, value, 0), 0)
    return found


def every(count, body):
    def step(index, carry):
        body(index)
        return carry

    lax.fori_loop(0, count, step, 0)


def kernel(n, nd, len_ref, q_hbm, k_hbm, v_hbm, g_hbm, w_hbm, dq_hbm, dk_hbm, dv_hbm, wg_hbm, *scratch):
    (
        q_buf, kv, far, near, t0, t1in, behind, relay, relay2, do_buf, dq_buf, o_buf, o_in,
        g_buf, g_mine, g_send, g_in, g_side, g_pass, g_far, w_buf, o_side, o_far, y_send, y_in, z_buf, z_in, acc, x_send, x_in, out_buf,
        q_l, kv_l, g_l, w_l, dq_s, out_s,
        far_s, far_r, near_s, near_r, t1_s, t1_r, ret_s, ret_r, rel_s, rel_r, rel2_s, rel2_r,
        o_s, o_r, oa_s, oa_r, of_s, of_r, g_s, g_r, wu_s, wd_s, w_r, wp_s, wp_r, y_s, y_r, z_s, z_r, x_s, x_r,
    ) = scratch
    f32, bf16 = jnp.float32, jnp.bfloat16
    i, z = lax.axis_index("seq"), lax.axis_index("dp")
    steps, _, _, tokens, _ = kv.shape
    per = steps // nd
    chips = n // 2
    chip = i // 2
    par = lax.rem(i, 2)
    mate = flip(i, 1)
    ahead, back = lax.rem(i + 2, n), lax.rem(i + n - 2, n)
    across = flip(i, n // 2)
    beside = flip(i, 2)
    relayed = n == 8
    assert steps == 8
    width = w_hbm.shape[1]
    half = width // 2
    own = width // n
    span = half // 2
    table = pair_order(nd, per)

    def pair_at(it):
        return pick(table, z, it)

    def rdma(src, dst, send, recv, **where):
        return pltpu.make_async_remote_copy(
            src_ref=src, dst_ref=dst, send_sem=send, recv_sem=recv, device_id=where, device_id_type=MESH
        )

    def columns(start, size):
        return pl.ds(pl.multiple_of(start, 128), size)

    def load_kv(it):
        at = pair_at(it) * PAIR
        for a in range(2):
            for b, ref in enumerate((k_hbm, v_hbm)):
                src = ref.at[:, columns(at + a * HEAD_DIM, HEAD_DIM)]
                pltpu.make_async_copy(src, kv.at[it, a, b], kv_l.at[it]).start()

    def load_q(it):
        at = pair_at(it) * PAIR
        for a in range(2):
            src = q_hbm.at[:, columns(at + a * HEAD_DIM, HEAD_DIM)]
            pltpu.make_async_copy(src, q_buf.at[it, a], q_l.at[it]).start()

    bits = []
    bit = n // 2
    while bit > 1:
        bits.append(bit)
        bit //= 2
    greet = [dict(seq=mate), dict(seq=ahead), dict(seq=back)]
    greet += [dict(seq=flip(i, b)) for b in bits]
    greet += [dict(dp=lax.rem(z + s, nd)) for s in range(1, nd)]
    barrier = pltpu.get_barrier_semaphore()
    for who in greet:
        pl.semaphore_signal(barrier, inc=1, device_id=who, device_id_type=MESH)

    every(steps, load_kv)
    load_g = pltpu.make_async_copy(g_hbm, g_buf, g_l.at[0])
    load_g.start()
    own_w = []
    for k in range(per):
        for h in range(2):
            src = w_hbm.at[pl.ds(k * PAIR, PAIR), pl.ds(h * half, half)]
            own_w.append(pltpu.make_async_copy(src, w_buf.at[z * per + k, h], w_l.at[2 * k + h]))
            own_w[-1].start()
    every(steps, load_q)

    @pl.when(chip == 0)
    def _():
        def clear(it):
            far[it] = jnp.zeros_like(far[it])

        every(steps, clear)

    with jax.named_scope("greet"):
        pl.semaphore_wait(barrier, len(greet))

    def far_copy(it, a):
        return rdma(kv.at[it, a], far.at[it, a], far_s.at[0], far_r.at[2 * it + a], seq=ahead)

    def far_relay_in(it):
        return rdma(kv.at[it, 1], relay.at[it], far_s.at[0], rel_r.at[it], seq=across)

    def far_relay_out(it):
        return rdma(relay.at[it], far.at[it, 1], rel_s.at[0], far_r.at[2 * it + 1], seq=beside)

    def ret_copy(it, a):
        return rdma(far.at[it, a], behind.at[it, a], ret_s.at[0], ret_r.at[2 * it + a], seq=back)

    def ret_relay_in(it):
        return rdma(far.at[it, 1], relay.at[it], ret_s.at[0], rel_r.at[it], seq=across)

    def ret_relay_out(it):
        return rdma(relay.at[it], behind.at[it, 1], rel_s.at[0], ret_r.at[2 * it + 1], seq=beside)

    def ret_relay2_in(it):
        return rdma(far.at[it, 0], relay2.at[it], ret_s.at[0], rel2_r.at[it], seq=beside)

    def ret_relay2_out(it):
        return rdma(relay2.at[it], behind.at[it, 0], rel2_s.at[it], ret_r.at[2 * it], seq=across)

    def shift_in(it):
        return rdma(far.at[it, 0], relay2.at[it], ret_s.at[0], rel2_r.at[it], seq=across)

    def shift_out(it):
        return rdma(relay2.at[it], behind.at[it, 0], rel2_s.at[it], ret_r.at[2 * it], seq=beside)

    def near_copy(src, it, a):
        return rdma(src.at[it, a], near.at[it, a], near_s.at[2 * it + a], near_r.at[2 * it + a], seq=mate)

    def t1_copy(it, a):
        return rdma(near.at[it, a], t1in.at[it, a], t1_s.at[0], t1_r.at[2 * it + a], seq=mate)

    def o_copy(it):
        return rdma(o_buf.at[it], o_in.at[it], o_s.at[0], o_r.at[it], seq=mate)

    def o_across(it):
        return rdma(o_buf.at[it], o_side.at[it], oa_s.at[0], oa_r.at[it], seq=across)

    def o_onward(it):
        return rdma(o_side.at[it], o_far.at[it], of_s.at[0], of_r.at[it], seq=mate)

    def y_copy(it):
        return rdma(y_send.at[it], y_in.at[it], y_s.at[0], y_r.at[it], seq=across)

    def w_up(piece):
        return rdma(w_buf.at[piece, par], w_buf.at[piece, par], wu_s.at[piece], w_r.at[piece], dp=lax.rem(z + 1, nd))

    def w_down(piece):
        return rdma(w_buf.at[piece, par], w_buf.at[piece, par], wd_s.at[piece], w_r.at[piece], dp=lax.rem(z + nd - 1, nd))

    def w_mate(piece, side):
        return rdma(w_buf.at[piece, side], w_buf.at[piece, side], wp_s.at[piece], wp_r.at[piece], seq=mate)

    def z_copy(it, source, shard):
        k = lax.rem(pair_at(it), per)
        return rdma(z_buf.at[it], z_in.at[source, k], z_s.at[it], z_r.at[source * per + k], dp=shard)

    def z_arrive(source, k):
        return rdma(z_buf.at[0], z_in.at[source, k], z_s.at[0], z_r.at[source * per + k], dp=source)

    def first_sends(it):
        with jax.named_scope("kv_load"):
            pltpu.make_async_copy(kv.at[it], kv.at[it], kv_l.at[it]).wait()

        @pl.when(chip < chips - 1)
        def _():
            far_copy(it, 0).start()
            if relayed:
                pl.when(chip != 1)(lambda: far_copy(it, 1).start())
                pl.when(chip == 1)(lambda: far_relay_in(it).start())
            else:
                far_copy(it, 1).start()

        @pl.when(par == 0)
        def _():
            for a in range(2):
                near_copy(kv, it, a).start()

    every(steps, first_sends)

    with jax.named_scope("w_load"):
        for copy in own_w:
            copy.wait()
    for k in range(per):
        pl.when(z < nd - 1)(lambda: w_up(z * per + k).start())
        pl.when(z > 0)(lambda: w_down(z * per + k).start())

    with jax.named_scope("g_load"):
        load_g.wait()
    at_row = i * tokens + lax.broadcasted_iota(jnp.int32, (tokens, 1), 0)
    live = at_row < len_ref[0]
    for c in range(chips):
        first = g_buf[:, 2 * c * own : (2 * c + 1) * own].astype(f32)
        second = g_buf[:, (2 * c + 1) * own : (2 * c + 2) * own].astype(f32)
        first, second = jnp.where(live, first, 0.0), jnp.where(live, second, 0.0)
        g_buf[:, 2 * c * own : (2 * c + 2) * own] = jnp.concatenate([first, second], 1).astype(bf16)
        g_mine[c * own : (c + 1) * own, :] = jnp.where(par == 0, first, second).T.astype(bf16)
        g_send[c * own : (c + 1) * own, :] = jnp.where(par == 0, second, first).T.astype(bf16)
    high = lax.rem(i // bits[0], 2)
    held = pl.ds(pl.multiple_of(high * span, span), span)
    given = pl.ds(pl.multiple_of((1 - high) * span, span), span)
    g_moves = [
        rdma(g_send, g_in, g_s.at[0], g_r.at[0], seq=mate),
        rdma(g_mine.at[given, :], g_side, g_s.at[1], g_r.at[1], seq=across),
        rdma(g_send.at[given, :], g_pass, g_s.at[2], g_r.at[2], seq=across),
    ]
    g_moves[0].start()

    @pl.when(high == 1)
    def _():
        for copy in g_moves[1:]:
            copy.start()

    g_moves.append(rdma(g_pass, g_far, g_s.at[3], g_r.at[3], seq=mate))

    def halo_relay(it):
        with jax.named_scope("hrel_wait"):
            far_relay_in(it).wait_recv()
        far_relay_out(it).start()

    if relayed:
        pl.when(chip == chips - 1)(lambda: halo_relay(0))

    scale = HEAD_DIM ** (-0.5)
    c_exp = scale * LOG2E

    def begin(it):
        @pl.when(chip > 0)
        def _():
            with jax.named_scope("far_wait"):
                for a in range(2):
                    far_copy(it, a).wait_recv()

        @pl.when(par == 1)
        def _():
            for a in range(2):
                near_copy(far, it, a).start()

        if relayed:
            for extra in range(2):
                at = 2 * it + extra

                @pl.when(jnp.logical_and(chip == chips - 1, jnp.logical_and(at > 0, at < steps)))
                def _():
                    halo_relay(at)

        piece = pair_at(it)

        @pl.when(piece // per != z)
        def _():
            with jax.named_scope("w_wait"):
                w_mate(piece, 1 - par).wait_recv()

        with jax.named_scope("do"):
            do = dot(g_buf[:, :half], w_buf[piece, 0], NT) + dot(g_buf[:, half:], w_buf[piece, 1], NT)
            do_buf[...] = do.astype(bf16)

    def give(m):
        with jax.named_scope("o_wait"):
            o_copy(m).wait_recv()

        @pl.when(high == 0)
        def _():
            with jax.named_scope("wgive"):
                part = dot(g_mine[given, :], o_buf[m], NN) + dot(g_in[given, :], o_in[m], NN)
                y_send[m] = part.astype(bf16)
            y_copy(m).start()

    def onward(m):
        @pl.when(high == 0)
        def _():
            with jax.named_scope("oa_wait"):
                o_across(m).wait_recv()
            o_onward(m).start()

    def combine(m):
        @pl.when(high == 0)
        def _():
            with jax.named_scope("of_wait"):
                o_onward(m).wait_recv()
            with jax.named_scope("wgrad"):
                total = dot(g_mine[held, :], o_buf[m], NN) + dot(g_in[held, :], o_in[m], NN)
                total = total + dot(g_side[...], o_side[m], NN) + dot(g_far[...], o_far[m], NN)
                place(m, total)

        @pl.when(high == 1)
        def _():
            with jax.named_scope("y_wait"):
                y_copy(m).wait_recv()
            with jax.named_scope("wgrad"):
                total = dot(g_mine[held, :], o_buf[m], NN) + dot(g_in[held, :], o_in[m], NN)
                place(m, total + y_in[m].astype(f32))

    def place(m, total):
        pair = pair_at(m)

        @pl.when(pair // per == z)
        def _():
            acc[lax.rem(pair, per)] = total

        @pl.when(pair // per != z)
        def _():
            z_buf[m] = total.astype(bf16)
            z_copy(m, z, pair // per).start()

    def pass_return(m):
        @pl.when(chip == chips - 1)
        def _():
            with jax.named_scope("rel2_wait"):
                ret_relay2_in(m).wait_recv()
            ret_relay2_out(m).start()

    def attend(it):
        causal_keys = lax.broadcasted_iota(jnp.int32, (tokens, tokens), 0)
        causal_queries = lax.broadcasted_iota(jnp.int32, (tokens, tokens), 1)
        for a in range(2):
            with jax.named_scope("near_wait"):
                near_copy(kv, it, a).wait_recv()
            q = q_buf[it, a]
            sources = (kv, near, far)
            parts, tops = [], []
            for offset, source in enumerate(sources):
                s = dot(source[it, a, 0], q, NT)
                if offset == 0:
                    s = jnp.where(causal_keys <= causal_queries, s, NEG)
                parts.append(s)
                top = jnp.max(s, axis=0, keepdims=True)
                if offset:
                    top = top + jnp.where(i >= offset, 0.0, NEG)
                tops.append(top)
            top = functools.reduce(jnp.maximum, tops) * c_exp
            total = None
            for offset in range(3):
                shift = top if offset == 0 else top + jnp.where(i >= offset, 0.0, -NEG)
                parts[offset] = jnp.exp2(parts[offset] * c_exp - shift)
                t = jnp.sum(parts[offset], axis=0, keepdims=True)
                total = t if total is None else total + t
            inverse = 1.0 / total
            out = None
            for offset, source in enumerate(sources):
                parts[offset] = parts[offset] * inverse
                o = dot(source[it, a, 1], parts[offset].astype(bf16), TN)
                out = o if out is None else out + o
            o = out.T.astype(bf16)
            o_buf[it, :, a * HEAD_DIM : (a + 1) * HEAD_DIM] = o
            do = do_buf[:, a * HEAD_DIM : (a + 1) * HEAD_DIM]
            delta = jnp.sum((do.astype(f32) * o.astype(f32)).T, axis=0, keepdims=True)
            near_copy(kv, it, a).wait_send()
            dq = None
            for offset, (source, term) in enumerate(zip(sources, (t0, near, far))):
                k, v = source[it, a, 0], source[it, a, 1]
                p = parts[offset]
                dv = dot(p.astype(bf16), do, NN)
                ds = (p * (dot(v, do, NT) - delta)).astype(bf16)
                dk = dot(ds, q, NN) * scale
                part = dot(k, ds, TN)
                dq = part if dq is None else dq + part
                term[it, a, 0] = dk.astype(bf16)
                term[it, a, 1] = dv.astype(bf16)
                if offset == 1:
                    t1_copy(it, a).start()
            dq_buf[it, :, a * HEAD_DIM : (a + 1) * HEAD_DIM] = (dq * scale).T.astype(bf16)
            if a == 0:
                pl.when(it < steps - 1)(lambda: move_weights(it))

                if relayed:
                    pl.when(it == steps - 1)(lambda: pass_return(0))

        o_copy(it).start()
        pl.when(high == 1)(lambda: o_across(it).start())
        pltpu.make_async_copy(dq_buf.at[it], dq_hbm.at[:, columns(pair_at(it) * PAIR, PAIR)], dq_s.at[0]).start()

    def move_weights(it):
        ends = jnp.logical_or(z == 0, z == nd - 1)
        j = it - jnp.where(ends, 1, 0)
        below, above = z - 1 - j // per, z + 1 + j // per

        @pl.when(jnp.logical_and(j >= 0, below >= 0))
        def _():
            piece = below * per + lax.rem(j, per)
            with jax.named_scope("up_wait"):
                w_up(piece).wait_recv()
            pl.when(z < nd - 1)(lambda: w_up(piece).start())
            w_mate(piece, par).start()

        @pl.when(jnp.logical_and(j >= 0, above <= nd - 1))
        def _():
            piece = above * per + lax.rem(j, per)
            with jax.named_scope("down_wait"):
                w_down(piece).wait_recv()
            pl.when(z > 0)(lambda: w_down(piece).start())
            w_mate(piece, par).start()

    def send_around(m):
        pl.when(m < steps - 1)(lambda: ret_relay2_in(m).start())
        ret_relay_in(m).start()
        pl.when(m == steps - 1)(lambda: shift_in(m).start())

    def stage_a(m):
        for a in range(2):
            with jax.named_scope("t1_wait"):
                t1_copy(m, a).wait_recv()

            @pl.when(par == 1)
            def _():
                far[m, a] = (far[m, a].astype(f32) + t1in[m, a].astype(f32)).astype(bf16)

        @pl.when(chip > 0)
        def _():
            if relayed:

                @pl.when(chip != 2)
                def _():
                    ret_copy(m, 0).start()
                    ret_copy(m, 1).start()

                pl.when(jnp.logical_and(chip == 2, m < steps - 2))(lambda: send_around(m))

            else:
                ret_copy(m, 0).start()
                ret_copy(m, 1).start()

    def corner_return(m):
        @pl.when(chip == 0)
        def _():
            with jax.named_scope("rel_wait"):
                ret_relay_in(m).wait_recv()
            ret_relay_out(m).start()

            @pl.when(jnp.int32(m) == steps - 1)
            def _():
                shift_in(m).wait_recv()
                shift_out(m).start()

    def step(it):
        pl.when(it == 4)(lambda: every(3, onward))
        pl.when(it > 4)(lambda: onward(it - 2))
        begin(it)

        @pl.when(it >= 1)
        def _():
            stage_a(it - 1)
            pl.when(it == 1)(g_moves[0].wait_recv)
            give(it - 1)

        @pl.when(jnp.logical_and(it == 4, high == 0))
        def _():
            g_moves[2].wait_recv()
            g_moves[3].start()

        @pl.when(it == 5)
        def _():
            @pl.when(high == 0)
            def _():
                g_moves[1].wait_recv()
                g_moves[3].wait_recv()

            every(3, combine)

        pl.when(it > 4)(lambda: combine(it - 2))
        if relayed:
            pl.when(it == steps - 2)(lambda: every(4, corner_return))
            pl.when(it == steps - 1)(lambda: corner_return(4))

        pltpu.make_async_copy(q_buf.at[it], q_buf.at[it], q_l.at[it]).wait()
        with jax.named_scope("attend"):
            attend(it)
        if relayed:
            pl.when(it == steps - 1)(lambda: pass_return(1))

    every(steps, step)
    first_left = steps - 2

    def trail(q):
        m = first_left + q
        onward(m)

        @pl.when(q == 0)
        def _():
            stage_a(steps - 1)
            give(steps - 1)

        if relayed:
            pl.when(jnp.logical_and(q == 0, chip == 2))(lambda: every(2, lambda r: send_around(steps - 2 + r)))
            pass_return(2 + q)
            pl.when(q == 0)(lambda: corner_return(5))
        combine(m)

    every(steps - first_left, trail)

    def finish(m):
        @pl.when(chip < chips - 1)
        def _():
            with jax.named_scope("ret_wait"):
                for a in range(2):
                    ret_copy(m, a).wait_recv()

        for a in range(2):
            for b, out in enumerate((dk_hbm, dv_hbm)):
                total = t0[m, a, b].astype(f32)
                total = total + jnp.where(par == 0, t1in[m, a, b].astype(f32), 0.0)
                total = total + jnp.where(chip < chips - 1, behind[m, a, b].astype(f32), 0.0)
                t0[m, a, b] = total.astype(bf16)
                dst = out.at[:, columns(pair_at(m) * PAIR + a * HEAD_DIM, HEAD_DIM)]
                pltpu.make_async_copy(t0.at[m, a, b], dst, out_s.at[0]).start()

    early = 3
    every(early, finish)
    if relayed:
        every(3, lambda q: pass_return(4 + q))
        every(2, lambda q: corner_return(6 + q))

    base = jnp.int32(0)
    rows = span
    levels = []
    for b in bits[1:]:
        rows //= 2
        up = lax.rem(i // b, 2)
        away = pl.ds(pl.multiple_of(base + (1 - up) * rows, rows), rows)
        base = base + up * rows
        levels.append((b, away, pl.ds(pl.multiple_of(base, rows), rows), pl.ds(span - 2 * rows, rows)))

    def x_copy(level, k):
        b, _, _, at = levels[level]
        sems = (x_s.at[level * per + k], x_r.at[level * per + k])
        return rdma(x_send.at[k, at, :], x_in.at[k, at, :], *sems, seq=flip(i, b))

    def x_start(level, k):
        _, away, _, at = levels[level]
        x_send[k, at, :] = acc[k, away, :].astype(bf16)
        x_copy(level, k).start()

    def x_finish(level, k):
        _, _, stay, at = levels[level]
        with jax.named_scope("x_wait"):
            x_copy(level, k).wait_recv()
        acc[k, stay, :] = acc[k, stay, :] + x_in[k, at, :].astype(f32)

    mine = pl.ds(pl.multiple_of(base, own), own)

    def put_copy(k):
        rows = pl.ds(k * PAIR, PAIR)
        return pltpu.make_async_copy(out_buf.at[rows, :], wg_hbm.at[rows, :], w_l.at[k])

    def deliver(k):
        out_buf[k * PAIR : (k + 1) * PAIR, :] = acc[k, mine, :].T
        put_copy(k).start()

    for k in range(per):
        for s in range(1, nd):
            source = lax.rem(z + s, nd)
            with jax.named_scope("z_wait"):
                z_arrive(source, k).wait_recv()
            acc[k] = acc[k] + z_in[source, k].astype(f32)
        if levels:
            x_start(0, k)
    every(steps - 1 - early, lambda m: finish(m + early))
    for level in range(len(levels)):
        for k in range(per):
            if level:
                x_start(level, k)
        for k in range(per):
            x_finish(level, k)
            if level == len(levels) - 1:
                deliver(k)
    finish(steps - 1)

    def sent(ref, sem):
        pltpu.make_async_copy(ref, ref, sem.at[0]).wait()

    pl.when(chip < chips - 1)(lambda: sent(kv, far_s))
    pl.when(chip > 0)(lambda: sent(far, ret_s))
    if relayed:
        pl.when(jnp.logical_or(chip == 0, chip == chips - 1))(lambda: sent(relay, rel_s))
    pl.when(high == 1)(lambda: sent(o_buf, oa_s))

    @pl.when(high == 0)
    def _():
        sent(o_side, of_s)
        sent(y_send, y_s)

    for ref, sem in ((near, t1_s), (o_buf, o_s), (dq_buf, dq_s), (t0, out_s)):
        sent(ref, sem)

    def settle(m):
        if relayed:
            pl.when(jnp.logical_and(chip == 0, m == steps - 1))(lambda: shift_out(m).wait_send())
            pl.when(jnp.logical_and(chip == chips - 1, m < steps - 1))(lambda: ret_relay2_out(m).wait_send())

        @pl.when(pair_at(m) // per != z)
        def _():
            z_copy(m, z, pair_at(m) // per).wait_send()
            w_mate(pair_at(m), par).wait_send()

        pl.when(jnp.logical_and(z < nd - 1, m < (z + 1) * per))(lambda: w_up(m).wait_send())
        pl.when(jnp.logical_and(z > 0, m >= z * per))(lambda: w_down(m).wait_send())

    with jax.named_scope("settle"):
        every(steps, settle)
    with jax.named_scope("rest"):
        g_moves[0].wait_send()

    @pl.when(high == 1)
    def _():
        g_moves[1].wait_send()
        g_moves[2].wait_send()

    pl.when(high == 0)(g_moves[3].wait_send)
    for level in range(len(levels)):
        for k in range(per):
            x_copy(level, k).wait_send()
    with jax.named_scope("put_wait"):
        for k in range(per):
            put_copy(k).wait()


def hand_over_kernel(*refs):
    count = len(refs) // 2
    for src, dst in zip(refs[:count], refs[count:]):
        dst[...] = src[...]


def hand_over(arrays, pieces):
    specs = [pl.BlockSpec((a.shape[0] // pieces, a.shape[1]), lambda p: (p, 0)) for a in arrays]
    return pl.pallas_call(
        hand_over_kernel,
        grid=(pieces,),
        in_specs=specs,
        out_specs=specs,
        out_shape=[jax.ShapeDtypeStruct(a.shape, a.dtype) for a in arrays],
        name="hand_over",
    )(*arrays)


def layer(n, nd, queries, keys, values, out_grad, proj_weight, lengths):
    f32, bf16 = jnp.float32, jnp.bfloat16
    tokens, feat = queries.shape[1:]
    rows, width = proj_weight.shape
    steps = feat // PAIR
    per = rows // PAIR
    half = width // 2
    span = half // 2
    own = width // n
    head = (steps, 2, tokens, HEAD_DIM)
    both = (steps, 2, 2, tokens, HEAD_DIM)
    pair = (steps, tokens, PAIR)
    levels = max(1, n.bit_length() - 3)
    vmem = [
        (head, bf16),
        *[(both, bf16)] * 6,
        *[((steps, 2, tokens, HEAD_DIM), bf16)] * 2,
        ((tokens, PAIR), bf16),
        *[(pair, bf16)] * 3,
        ((tokens, width), bf16),
        *[((half, tokens), bf16)] * 3,
        *[((span, tokens), bf16)] * 3,
        ((steps, 2, PAIR, half), bf16),
        *[(pair, bf16)] * 2,
        *[((steps, span, PAIR), bf16)] * 3,
        ((nd, per, span, PAIR), bf16),
        ((per, span, PAIR), f32),
        *[((per, span, PAIR), bf16)] * 2,
        ((rows, own), f32),
    ]
    sems = [steps, steps, 1, 2 * per, 1, 1]
    sems += [1, 2 * steps, 2 * steps, 2 * steps, 1, 2 * steps, 1, 2 * steps, 1] + [steps] * 3
    sems += [1, steps] * 3 + [4, 4] + [steps] * 5 + [1, steps, steps] + [nd * per] + [levels * per] * 2
    anywhere = pl.BlockSpec(memory_space=pl.ANY)
    grad = jax.ShapeDtypeStruct((tokens, feat), bf16)
    dq, dk, dv, wg = pl.pallas_call(
        functools.partial(kernel, n, nd),
        in_specs=[pl.BlockSpec(memory_space=pltpu.SMEM)] + [anywhere] * 5,
        out_specs=[anywhere] * 4,
        out_shape=[grad, grad, grad, jax.ShapeDtypeStruct((rows, own), f32)],
        scratch_shapes=[pltpu.VMEM(*spec) for spec in vmem] + [pltpu.SemaphoreType.DMA((s,)) for s in sems],
        compiler_params=pltpu.CompilerParams(
            collective_id=0, has_side_effects=True, vmem_limit_bytes=67043328
        ),
        name="banded_backward",
    )(lengths, queries[0], keys[0], values[0], out_grad[0], proj_weight)
    dq, dk, dv, wg = hand_over((dq, dk, dv, wg), 2)
    return dq[None], dk[None], dv[None], wg


def solution(mesh):
    rows = P("dp", "seq", None)
    return jax.shard_map(
        functools.partial(layer, mesh.shape["seq"], mesh.shape["dp"]),
        mesh=mesh,
        in_specs=(rows, rows, rows, rows, P("dp", None), P("dp")),
        out_specs=(rows, rows, rows, P("dp", "seq")),
        check_vma=False,
    )
```
